256 devices in a mesh: dp: 8 (over x_lo, y), mp: 32 (over z, x_hi, core).
Axes of the slice: x: 4 (x_hi: 2, x_lo: 2; x = x_hi * 2 + x_lo), y: 4, z: 8, core: 2. Of those that a mesh axis runs over, the one named last changes fastest.
Arguments:
- tokens: bfloat16 [1024, 6144], P(('dp', 'mp')), may hold values from -6 to 6
- norm_gain: float32 [6144], replicated, may hold values from 0.5 to 1.5
- w_query: bfloat16 [6144, 4096], P('dp', 'mp'), as said below
- w_key: bfloat16 [6144, 4096], P('dp', 'mp'), as said below
- w_value: bfloat16 [6144, 4096], P('dp', 'mp'), may hold values from -0.078125 to 0.078125
- w_inner: bfloat16 [6144, 24576], P('dp', 'mp'), may hold values from -0.078125 to 0.078125
- bias_inner: float32 [24576], P('mp'), may hold values from -3 to 3
- w_attn_out: bfloat16 [4096, 6144], P('mp', 'dp'), may hold values from -0.09375 to 0.09375
- w_outer: bfloat16 [24576, 6144], P('mp', 'dp'), may hold values from -0.0390625 to 0.0390625
- temper: float32 [32], P('mp'), may hold values from 0.5 to 24
Outputs:
- result: bfloat16 [1024, 6144], P(('dp', 'mp'))
The draws below stay inside these ranges and needn't reach their ends.
Inputs may be any that keep to these rules, and one draw needn't show every extreme that they name: `w_query`: entries of order 6144 ** -0.5. `w_key`: entries of order 6144 ** -0.5.
All inputs are finite; a program needn't handle non-finite values.
Results may differ from the reference program's by a relative error of at most 0.023.
Values may be sent and summed in bfloat16 or wider, within the bound.
A program may use at most 64 MiB of HBM per device.

```python
import math
import jax
import jax.numpy as jnp
from jax import lax

D = 6144
HEADS = 32
HEAD = 128
FF = 24576
HD = 4096
PATCHES = 128
TOKENS = 1024
N_DP = 8


def shared_draws(key):
    key_query = jax.random.fold_in(key, 11)
    key_noise = jax.random.fold_in(key, 12)
    key_temper = jax.random.fold_in(key, 14)
    scale = D ** (-0.5)
    limit = 6.0 * scale
    query = jnp.clip(jax.random.normal(key_query, (D, HD), jnp.float32) * scale, -limit, limit)
    noise = jnp.clip(jax.random.normal(key_noise, (D, HD), jnp.float32) * scale, -limit, limit)
    temper = jnp.exp(jax.random.uniform(key_temper, (HEADS,), jnp.float32, jnp.log(0.5), jnp.log(6.0)))
    keys = noise
    return (query, keys, temper)


def draw_w_query(key, part):
    return shared_draws(key)[0].astype(jnp.bfloat16)


def draw_w_key(key, part):
    return shared_draws(key)[1].astype(jnp.bfloat16)


def draw_temper(key, part):
    return shared_draws(key)[2]


def level_of(rng, extent, split, low, high):
    level, own = 1.0, jax.random.fold_in(rng, 6)
    for dim, blocks in split:
        heights = jnp.exp(jax.random.uniform(jax.random.fold_in(own, dim), (blocks,), jnp.float32, low / len(split), high / len(split)))
        level = level * jnp.repeat(heights, extent[dim] // blocks).reshape([-1 if axis == dim else 1 for axis in range(len(extent))])
    return level


def bell_draw(stream_key, extent, deviation, most, shards=(), kind=jnp.bfloat16):
    result = deviation * jax.random.normal(stream_key, extent, jnp.float32)
    if shards:
        result = result * level_of(stream_key, extent, shards, -0.22, 0.18)
    return jnp.clip(result, -most, most).astype(kind)


def setup_inputs(seed: int = 0) -> dict:
    streams_of = jax.random.split(jax.random.key(seed), 11)
    return {
        "tokens": bell_draw(streams_of[0], (TOKENS, D), 1.0, 6.0, ((0, 256),)),
        "norm_gain": jnp.clip(1.0 + 0.1 * jax.random.normal(streams_of[1], (D,), jnp.float32), 0.5, 1.5),
        "w_query": draw_w_query(jax.random.fold_in(streams_of[10], 71), 0),
        "w_key": draw_w_key(jax.random.fold_in(streams_of[10], 71), 0),
        "w_value": bell_draw(streams_of[4], (D, HD), D ** -0.5, 0.078125, ((0, 8), (1, 32))),
        "w_inner": bell_draw(streams_of[5], (D, FF), D ** -0.5, 0.078125, ((0, 8), (1, 32))),
        "bias_inner": bell_draw(streams_of[6], (FF,), 0.5, 3.0, ((0, 32),), jnp.float32),
        "w_attn_out": bell_draw(streams_of[7], (HD, D), HD ** -0.5, 0.09375, ((0, 32), (1, 8))),
        "w_outer": bell_draw(streams_of[8], (FF, D), FF ** -0.5, 0.0390625, ((0, 32), (1, 8))),
        "temper": draw_temper(jax.random.fold_in(streams_of[10], 71), 0),
    }


def normalize(values):
    center = values - lax.optimization_barrier(jnp.mean(values, axis=-1, keepdims=True))
    spread = lax.optimization_barrier(jnp.mean(center * center, axis=-1, keepdims=True))
    return center * lax.rsqrt(spread + 1e-06)

def reference(tokens, norm_gain, w_query, w_key, w_value, w_inner, bias_inner, w_attn_out, w_outer, temper):
    local = tokens.astype(jnp.float32)
    normed = (normalize(local) * norm_gain.astype(jnp.float32)).astype(jnp.bfloat16)
    query = jnp.dot(normed, w_query, preferred_element_type=jnp.float32).astype(jnp.bfloat16)
    keys = jnp.dot(normed, w_key, preferred_element_type=jnp.float32).astype(jnp.bfloat16)
    values = jnp.dot(normed, w_value, preferred_element_type=jnp.float32).astype(jnp.bfloat16)
    shape = (N_DP, PATCHES, HEADS, HEAD)
    query_norm = normalize(query.astype(jnp.float32).reshape(shape)).astype(jnp.bfloat16)
    key_norm = normalize(keys.astype(jnp.float32).reshape(shape)).astype(jnp.bfloat16)
    values4 = values.reshape(shape).astype(jnp.float32)
    scale = temper.astype(jnp.float32) / math.sqrt(HEAD)
    scores = jnp.einsum('bqhc,bkhc->bhqk', query_norm.astype(jnp.float32), key_norm.astype(jnp.float32))
    scores = scores * scale[None, :, None, None]
    probs = jax.nn.softmax(scores, axis=-1).astype(jnp.bfloat16)
    mixed = jnp.einsum('bhqk,bkhc->bqhc', probs.astype(jnp.float32), values4)
    mixed = mixed.astype(jnp.bfloat16).reshape(TOKENS, HD)
    inner = jnp.dot(normed, w_inner, preferred_element_type=jnp.float32) + bias_inner.astype(jnp.float32)
    activ = jax.nn.gelu(inner, approximate=False).astype(jnp.bfloat16)
    total = jnp.dot(mixed, w_attn_out, preferred_element_type=jnp.float32)
    total = total + jnp.dot(activ, w_outer, preferred_element_type=jnp.float32)
    return (local + total).astype(jnp.bfloat16)
```

```python
import math

import jax
import jax.numpy as jnp
from jax import lax
from jax.experimental import pallas as pl
from jax.experimental.pallas import tpu as pltpu
from jax.sharding import PartitionSpec as P

HEAD = 128
IMAGES = 8
PLANES = 8
ROWS = 4
WIDTH = 768
BLOCK = 128
STRIP = 16
HIDDEN = 768
FIRST = 3 * HEAD + HIDDEN
SECOND = HEAD + HIDDEN
OFFSETS = (1, -1, 2, -2, 3, -3, 4)
MESH = pl.DeviceIdType.MESH
F32 = jnp.float32
BF16 = jnp.bfloat16


def offset_of(step):
    return ((step + 1) // 2) * (2 * (step % 2) - 1)


def normalize(values):
    center = values - jnp.mean(values, axis=-1, keepdims=True)
    spread = jnp.mean(center * center, axis=-1, keepdims=True)
    return center * lax.rsqrt(spread + 1e-06)


def gathered_row(place):
    image, within = place >> 4, place & 15
    return ((within >> 2) & 1) * 64 + (within >> 3) * 32 + image * 4 + (within & 3)


def to_strips():
    row = lax.broadcasted_iota(jnp.int32, (BLOCK, BLOCK), 0)
    column = lax.broadcasted_iota(jnp.int32, (BLOCK, BLOCK), 1)
    return jnp.where(column == gathered_row(row), 1.0, 0.0).astype(BF16)


def from_strips():
    row = lax.broadcasted_iota(jnp.int32, (BLOCK, BLOCK), 0)
    column = lax.broadcasted_iota(jnp.int32, (BLOCK, BLOCK), 1)
    return jnp.where(row == gathered_row(column), 1.0, 0.0).astype(BF16)


def kernel(
    tokens,
    gain,
    w_query,
    w_key,
    w_value,
    w_inner,
    bias,
    w_attn_out,
    w_outer,
    temper,
    out,
    first,
    second,
    norm_out,
    norm_in,
    lines,
    planes,
    part_out,
    part_in,
    strips,
    acts,
    pair_own,
    pair_out,
    pair_in,
    plane_out,
    plane_in,
    cross_out,
    cross_in,
    final_out,
    final_in,
    w_sem,
    norm_sem,
    x_sem,
    z_sem,
    core_sem,
    part_sem,
    acts_sem,
    pair_sem,
    plane_sem,
    cross_sem,
    final_sem,
):
    dp = lax.axis_index("dp")
    mp = lax.axis_index("mp")
    z, lane = mp // 4, mp % 4
    x_hi, core = lane // 2, lane % 2
    other_core = (dp, mp + 1 - 2 * core)
    other_x = (dp, mp + 2 - 4 * x_hi)

    def plane_device(plane):
        return (dp, plane * 4 + lane)

    def around(offset):
        return lax.rem(z + offset + PLANES, PLANES)

    def image_at(step):
        return lax.rem(dp + step, IMAGES)

    def image_before(step):
        return lax.rem(dp - step + IMAGES, IMAGES)

    def send(source, target, sems, index, device):
        return pltpu.make_async_remote_copy(
            src_ref=source,
            dst_ref=target,
            send_sem=sems.at[(0, *index)],
            recv_sem=sems.at[(1, *index)],
            device_id=device,
            device_id_type=MESH,
        )

    weights = [
        pltpu.make_async_copy(w_query, first.at[:, pl.ds(0, HEAD)], w_sem.at[0]),
        pltpu.make_async_copy(w_key, first.at[:, pl.ds(HEAD, HEAD)], w_sem.at[1]),
        pltpu.make_async_copy(w_value, first.at[:, pl.ds(2 * HEAD, HEAD)], w_sem.at[2]),
        pltpu.make_async_copy(w_inner, first.at[:, pl.ds(3 * HEAD, HIDDEN)], w_sem.at[3]),
        pltpu.make_async_copy(w_attn_out, second.at[pl.ds(0, HEAD), :], w_sem.at[4]),
        pltpu.make_async_copy(w_outer, second.at[pl.ds(HEAD, HIDDEN), :], w_sem.at[5]),
    ]
    barrier = pltpu.get_barrier_semaphore()
    peers = [(image_at(step), mp) for step in range(1, IMAGES)]
    peers += [plane_device(around(offset)) for offset in OFFSETS]
    peers += [other_core, other_x]
    for peer in peers:
        pl.semaphore_signal(barrier, inc=1, device_id=peer, device_id_type=MESH)
    for copy in weights:
        copy.start()

    normed = (normalize(tokens[...].astype(F32)) * gain[...]).astype(BF16)
    for block in range(IMAGES):
        norm_out[block] = normed[:, block * WIDTH : (block + 1) * WIDTH]
    pl.semaphore_wait(barrier, len(peers))

    def norm_copy(step):
        return send(norm_out.at[image_at(step)], norm_in.at[dp], norm_sem, (step,), (image_at(step), mp))

    def norm_landed(step):
        place = norm_in.at[image_before(step)]
        return send(place, place, norm_sem, (step,), (image_before(step), mp))

    for step in range(1, IMAGES):
        norm_copy(step).start()
    norm_in[dp] = norm_out[dp]
    for step in range(1, IMAGES):
        norm_landed(step).wait_recv()
    for image in range(IMAGES):
        lines[pl.ds(image * ROWS, ROWS), :] = norm_in[image].astype(F32)
    planes[z, core, x_hi] = lines[...].astype(BF16)

    def x_copy(side):
        place = planes.at[z, core, side]
        return send(place, place, x_sem, (), other_x)

    def z_copy(side, step):
        place = planes.at[z, core, side]
        return send(place, place, z_sem, (side, step), plane_device(around(OFFSETS[step])))

    def z_landed(side, step, plane):
        place = planes.at[plane, core, side]
        return send(place, place, z_sem, (side, step), plane_device(plane))

    def core_copy(plane, side):
        place = planes.at[plane, side]
        return send(place, place, core_sem, (plane,), other_core)

    x_copy(x_hi).start()
    for step in range(len(OFFSETS)):
        z_copy(x_hi, step).start()
    x_copy(1 - x_hi).wait_recv()
    for step in range(len(OFFSETS)):
        z_copy(1 - x_hi, step).start()
    core_copy(z, core).start()
    for copy in weights[:4]:
        copy.wait()

    def part_copy(plane, step):
        image = image_at(step)
        return send(part_out.at[plane, image], part_in.at[plane, dp], part_sem, (plane, step), (image, mp))

    def part_landed(plane, step):
        image = image_before(step)
        place = part_in.at[plane, image]
        return send(place, place, part_sem, (plane, step), (image, mp))

    def project(step, carry):
        @pl.when(step + 1 < PLANES)
        def _():
            plane = around(-offset_of(step + 1))
            z_landed(x_hi, step, plane).wait_recv()
            z_landed(1 - x_hi, step, plane).wait_recv()
            core_copy(plane, core).start()

        plane = around(-offset_of(step))
        core_copy(plane, 1 - core).wait_recv()
        rows = jnp.dot(
            to_strips(), planes[plane].reshape(BLOCK, WIDTH), preferred_element_type=F32
        ).astype(BF16)
        part = jnp.dot(rows, first[...], preferred_element_type=F32).astype(BF16)
        part_out[plane] = part.reshape(IMAGES, STRIP, FIRST)

        def go(ahead, carry):
            part_copy(plane, ahead).start()
            return carry

        return lax.fori_loop(1, IMAGES, go, carry)

    lax.fori_loop(0, PLANES, project, 0)

    def collect(step, carry):
        plane = around(-offset_of(step))

        def landed(ahead, carry):
            part_landed(plane, ahead).wait_recv()
            return carry

        lax.fori_loop(1, IMAGES, landed, 0)
        part_in[plane, dp] = part_out[plane, dp]
        total = part_in[plane, 0].astype(F32)
        for image in range(1, IMAGES):
            total += part_in[plane, image].astype(F32)
        strips[plane] = total[:, : 3 * HEAD].astype(BF16).astype(F32)
        inner = total[:, 3 * HEAD :] + bias[...]
        activ = 0.5 * inner * (1.0 + lax.erf(inner * math.sqrt(0.5)))
        acts[plane, dp, :, HEAD:] = activ.astype(BF16)
        return carry

    lax.fori_loop(0, PLANES, collect, 0)

    whole = strips[...].reshape(BLOCK, 3 * HEAD)
    query_norm = normalize(whole[:, :HEAD]).astype(BF16)
    key_norm = normalize(whole[:, HEAD : 2 * HEAD]).astype(BF16)
    scores = lax.dot_general(
        query_norm, key_norm, (((1,), (1,)), ((), ())), preferred_element_type=F32
    ) * (temper[...] / math.sqrt(HEAD))
    weight = jnp.exp(scores - jnp.max(scores, axis=-1, keepdims=True))
    probs = (weight / jnp.sum(weight, axis=-1, keepdims=True)).astype(BF16)
    mixed = jnp.dot(probs, whole[:, 2 * HEAD :].astype(BF16), preferred_element_type=F32)
    mixed = mixed.astype(BF16).reshape(PLANES, STRIP, HEAD)
    for plane in range(PLANES):
        acts[plane, dp, :, :HEAD] = mixed[plane]

    def acts_copy(plane, step):
        place = acts.at[plane, dp]
        return send(place, place, acts_sem, (plane, step), (image_at(step), mp))

    def acts_landed(plane, step):
        image = image_before(step)
        place = acts.at[plane, image]
        return send(place, place, acts_sem, (plane, step), (image, mp))

    def spread(step, carry):
        plane = around(offset_of(PLANES - 1 - step))

        def go(ahead, carry):
            acts_copy(plane, ahead).start()
            return carry

        return lax.fori_loop(1, IMAGES, go, carry)

    lax.fori_loop(0, PLANES, spread, 0)
    for copy in weights[4:]:
        copy.wait()

    def pair_copy(plane):
        return send(pair_out.at[plane], pair_in.at[plane], pair_sem, (plane,), other_core)

    def plane_copy(plane, slot):
        return send(plane_out.at[plane], plane_in.at[slot], plane_sem, (slot,), plane_device(plane))

    def plane_landed(slot):
        place = plane_in.at[slot]
        return send(place, place, plane_sem, (slot,), plane_device(around(-offset_of(slot + 1))))

    def pass_on(slot, plane):
        pair_copy(plane).wait_recv()
        total = pair_own[plane] + pair_in[plane].astype(F32)
        pair_own[plane] = total
        plane_out[plane] = total.astype(BF16)

    def output(step, carry):
        @pl.when(step < PLANES)
        def _():
            plane = around(offset_of(PLANES - 1 - step))

            def landed(ahead, carry):
                acts_landed(plane, ahead).wait_recv()
                return carry

            lax.fori_loop(1, IMAGES, landed, 0)
            rows = jnp.dot(
                from_strips(), acts[plane].reshape(BLOCK, SECOND), preferred_element_type=F32
            ).astype(BF16)
            part = jnp.dot(rows, second[...], preferred_element_type=F32).reshape(2, 64, WIDTH)
            low, high = part[0], part[1]
            pair_own[plane] = jnp.where(core == 0, low, high)
            pair_out[plane] = jnp.where(core == 0, high, low).astype(BF16)
            pair_copy(plane).start()

        @pl.when(step >= 1)
        def _():
            slot = PLANES - 1 - step
            plane = around(offset_of(slot + 1))
            pass_on(slot, plane)

            @pl.when(step < PLANES)
            def _():
                plane_copy(plane, slot).start()

        return carry

    lax.fori_loop(0, PLANES + 1, output, 0)
    total = pair_own[z]
    for slot in reversed(range(PLANES - 1)):
        plane_landed(slot).wait_recv()
        total += plane_in[slot].astype(F32)
    sides = total.reshape(2, 32, WIDTH)
    mine = jnp.where(x_hi == 0, sides[0], sides[1])
    cross_out[...] = jnp.where(x_hi == 0, sides[1], sides[0]).astype(BF16)
    cross = send(cross_out, cross_in, cross_sem, (), other_x)
    cross.start()
    cross.wait_recv()
    lines[...] = mine + cross_in[...].astype(F32)
    for image in range(IMAGES):
        final_out[image] = lines[pl.ds(image * ROWS, ROWS), :].astype(BF16)

    def final_copy(step):
        return send(final_out.at[image_at(step)], final_in.at[dp], final_sem, (step,), (image_at(step), mp))

    def final_landed(step):
        place = final_in.at[image_before(step)]
        return send(place, place, final_sem, (step,), (image_before(step), mp))

    for step in range(1, IMAGES):
        final_copy(step).start()
    final_in[dp] = final_out[dp]
    for step in range(1, IMAGES):
        final_landed(step).wait_recv()
    for block in range(IMAGES):
        columns = pl.ds(block * WIDTH, WIDTH)
        out[:, columns] = (tokens[:, columns].astype(F32) + final_in[block].astype(F32)).astype(BF16)

    for step in range(1, IMAGES):
        norm_copy(step).wait_send()
        final_copy(step).wait_send()
    x_copy(x_hi).wait_send()
    cross.wait_send()
    for step in range(len(OFFSETS)):
        z_copy(x_hi, step).wait_send()
        z_copy(1 - x_hi, step).wait_send()

    def sent(plane, carry):
        core_copy(plane, core).wait_send()
        pair_copy(plane).wait_send()

        def one(ahead, carry):
            part_copy(plane, ahead).wait_send()
            acts_copy(plane, ahead).wait_send()
            return carry

        return lax.fori_loop(1, IMAGES, one, carry)

    lax.fori_loop(0, PLANES, sent, 0)
    for slot in range(PLANES - 1):
        plane_copy(around(offset_of(slot + 1)), slot).wait_send()


def per_device(
    tokens, norm_gain, w_query, w_key, w_value, w_inner, bias_inner, w_attn_out, w_outer, temper
):
    vmem = pl.BlockSpec(memory_space=pltpu.VMEM)
    anywhere = pl.BlockSpec(memory_space=pl.ANY)
    dma = pltpu.SemaphoreType.DMA
    return pl.pallas_call(
        kernel,
        out_shape=jax.ShapeDtypeStruct(tokens.shape, BF16),
        in_specs=[vmem, vmem, anywhere, anywhere, anywhere, anywhere, vmem, anywhere, anywhere, vmem],
        out_specs=vmem,
        scratch_shapes=[
            pltpu.VMEM((WIDTH, FIRST), BF16),
            pltpu.VMEM((SECOND, WIDTH), BF16),
            pltpu.VMEM((IMAGES, ROWS, WIDTH), BF16),
            pltpu.VMEM((IMAGES, ROWS, WIDTH), BF16),
            pltpu.VMEM((32, WIDTH), F32),
            pltpu.VMEM((PLANES, 2, 2, 32, WIDTH), BF16),
            pltpu.VMEM((PLANES, IMAGES, STRIP, FIRST), BF16),
            pltpu.VMEM((PLANES, IMAGES, STRIP, FIRST), BF16),
            pltpu.VMEM((PLANES, STRIP, 3 * HEAD), F32),
            pltpu.VMEM((PLANES, IMAGES, STRIP, SECOND), BF16),
            pltpu.VMEM((PLANES, 64, WIDTH), F32),
            pltpu.VMEM((PLANES, 64, WIDTH), BF16),
            pltpu.VMEM((PLANES, 64, WIDTH), BF16),
            pltpu.VMEM((PLANES, 64, WIDTH), BF16),
            pltpu.VMEM((PLANES - 1, 64, WIDTH), BF16),
            pltpu.VMEM((32, WIDTH), BF16),
            pltpu.VMEM((32, WIDTH), BF16),
            pltpu.VMEM((IMAGES, ROWS, WIDTH), BF16),
            pltpu.VMEM((IMAGES, ROWS, WIDTH), BF16),
            dma((6,)),
            dma((2, IMAGES)),
            dma((2,)),
            dma((2, 2, PLANES - 1)),
            dma((2, PLANES)),
            dma((2, PLANES, IMAGES)),
            dma((2, PLANES, IMAGES)),
            dma((2, PLANES)),
            dma((2, PLANES - 1)),
            dma((2,)),
            dma((2, IMAGES)),
        ],
        compiler_params=pltpu.CompilerParams(
            collective_id=0, has_side_effects=True, vmem_limit_bytes=48 * 1024 * 1024
        ),
    )(
        tokens,
        norm_gain.reshape(1, -1),
        w_query,
        w_key,
        w_value,
        w_inner,
        bias_inner.reshape(1, -1),
        w_attn_out,
        w_outer,
        temper.reshape(1, 1),
    )


def solution(mesh):
    return jax.shard_map(
        per_device,
        mesh=mesh,
        in_specs=(
            P(("dp", "mp"), None),
            P(),
            P("dp", "mp"),
            P("dp", "mp"),
            P("dp", "mp"),
            P("dp", "mp"),
            P("mp"),
            P("mp", "dp"),
            P("mp", "dp"),
            P("mp"),
        ),
        out_specs=P(("dp", "mp"), None),
        check_vma=False,
    )
```

```python
import math

import jax
import jax.numpy as jnp
from jax import lax
from jax.experimental import pallas as pl
from jax.experimental.pallas import tpu as pltpu
from jax.sharding import PartitionSpec as P

HEAD = 128
IMAGES = 8
STACK = 4
PLANES = 8
ROWS = 4
WIDTH = 768
BLOCK = 128
STRIP = 16
HIDDEN = 768
FIRST = 3 * HEAD + HIDDEN
X_FIRST = 640
Y_FIRST = FIRST - X_FIRST
SECOND = HEAD + HIDDEN
LAG = 2
X_ACTS = 512
MESH = pl.DeviceIdType.MESH
F32 = jnp.float32
BF16 = jnp.bfloat16


def offset_of(step):
    return ((step + 1) // 2) * (2 * (step % 2) - 1)


def normalize(values):
    center = values - jnp.mean(values, axis=-1, keepdims=True)
    spread = jnp.mean(center * center, axis=-1, keepdims=True)
    return center * lax.rsqrt(spread + 1e-06)


def gathered_row(place):
    image, within = place >> 4, place & 15
    return ((within >> 2) & 1) * 64 + (within >> 3) * 32 + image * 4 + (within & 3)


def to_strips():
    row = lax.broadcasted_iota(jnp.int32, (BLOCK, BLOCK), 0)
    column = lax.broadcasted_iota(jnp.int32, (BLOCK, BLOCK), 1)
    return jnp.where(column == gathered_row(row), 1.0, 0.0).astype(BF16)


def from_strips():
    row = lax.broadcasted_iota(jnp.int32, (BLOCK, BLOCK), 0)
    column = lax.broadcasted_iota(jnp.int32, (BLOCK, BLOCK), 1)
    return jnp.where(row == gathered_row(column), 1.0, 0.0).astype(BF16)


def kernel(
    tokens_hbm,
    gain_hbm,
    w_query,
    w_key,
    w_value,
    w_inner,
    bias_hbm,
    w_attn_out,
    w_outer,
    temper,
    out,
    tokens,
    gain,
    bias,
    first,
    second,
    norm_out,
    norm_in,
    lines,
    planes,
    part,
    part_x,
    mid_x,
    fin_x,
    part_y,
    mid_y,
    keep_y,
    fin_y,
    strips,
    acts,
    pair_own,
    pair_out,
    pair_in,
    plane_out,
    plane_in,
    final_out,
    final_in,
    w_sem,
    norm_sem,
    z_sem,
    core_sem,
    part_sem,
    acts_sem,
    pair_sem,
    plane_sem,
    final_sem,
):
    dp = lax.axis_index("dp")
    mp = lax.axis_index("mp")
    z, lane = mp // 4, mp % 4
    x_hi, core = lane // 2, lane % 2
    x_lo, y = dp // STACK, dp % STACK
    other_core = (dp, mp + 1 - 2 * core)
    other_x_lo = ((1 - x_lo) * STACK + y, mp)

    def plane_device(plane):
        return (dp, plane * 4 + lane)

    def around(offset):
        return lax.rem(z + offset + PLANES, PLANES)

    def image_at(step):
        return lax.rem(dp + step, IMAGES)

    def image_before(step):
        return lax.rem(dp - step + IMAGES, IMAGES)

    def y_at(step):
        return lax.rem(y + step, STACK)

    def y_before(step):
        return lax.rem(y - step + STACK, STACK)

    def y_device(row):
        return (x_lo * STACK + row, mp)

    def send(source, target, sems, index, device):
        return pltpu.make_async_remote_copy(
            src_ref=source,
            dst_ref=target,
            send_sem=sems.at[(0, *index)],
            recv_sem=sems.at[(1, *index)],
            device_id=device,
            device_id_type=MESH,
        )

    weights = [
        pltpu.make_async_copy(tokens_hbm, tokens, w_sem.at[6]),
        pltpu.make_async_copy(gain_hbm, gain, w_sem.at[7]),
        pltpu.make_async_copy(w_query, first.at[:, pl.ds(0, HEAD)], w_sem.at[0]),
        pltpu.make_async_copy(w_key, first.at[:, pl.ds(HEAD, HEAD)], w_sem.at[1]),
        pltpu.make_async_copy(w_value, first.at[:, pl.ds(2 * HEAD, HEAD)], w_sem.at[2]),
        pltpu.make_async_copy(w_inner, first.at[:, pl.ds(3 * HEAD, HIDDEN)], w_sem.at[3]),
        pltpu.make_async_copy(bias_hbm, bias, w_sem.at[8]),
        pltpu.make_async_copy(w_attn_out, second.at[pl.ds(0, HEAD), :], w_sem.at[4]),
        pltpu.make_async_copy(w_outer, second.at[pl.ds(HEAD, HIDDEN), :], w_sem.at[5]),
    ]
    for copy in weights[:2]:
        copy.start()
    pieces = [(step, flip) for step in range(IMAGES) for flip in range(2) if step or flip]

    def half(flip):
        return (1 - x_hi) if flip else x_hi

    def half_mp(flip):
        return z * 4 + half(flip) * 2 + core

    barrier = pltpu.get_barrier_semaphore()
    peers = [plane_device(around(offset_of(step))) for step in reversed(range(1, PLANES))]
    peers += [(image_at(step), half_mp(flip)) for step, flip in pieces] + [other_core]
    for peer in peers:
        pl.semaphore_signal(barrier, inc=1, device_id=peer, device_id_type=MESH)
    for copy in weights[2:]:
        copy.start()
    for copy in weights[:2]:
        copy.wait()

    normed = (normalize(tokens[...].astype(F32)) * gain[...]).astype(BF16)
    for block in range(IMAGES):
        norm_out[block] = normed[:, block * WIDTH : (block + 1) * WIDTH]
    pl.semaphore_wait(barrier, len(peers))

    def norm_copy(step, flip):
        return send(
            norm_out.at[image_at(step)],
            norm_in.at[dp, x_hi],
            norm_sem,
            (step, flip),
            (image_at(step), half_mp(flip)),
        )

    def norm_landed(step, flip):
        place = norm_in.at[image_before(step), half(flip)]
        return send(place, place, norm_sem, (step, flip), (image_before(step), half_mp(flip)))

    for piece in pieces:
        norm_copy(*piece).start()
    norm_in[dp, x_hi] = norm_out[dp]
    for piece in pieces:
        norm_landed(*piece).wait_recv()
    for side in range(2):
        for image in range(IMAGES):
            lines[pl.ds(side * 32 + image * ROWS, ROWS), :] = norm_in[image, side].astype(F32)
    planes[z, core] = lines[...].astype(BF16)

    def z_copy(step):
        place = planes.at[z, core]
        return send(place, place, z_sem, (step,), plane_device(around(offset_of(step))))

    def z_landed(step):
        plane = around(-offset_of(step))
        place = planes.at[plane, core]
        return send(place, place, z_sem, (step,), plane_device(plane))

    def core_copy(plane, side):
        place = planes.at[plane, side]
        return send(place, place, core_sem, (plane,), other_core)

    core_copy(z, core).start()
    for step in range(1, PLANES):
        z_copy(step).start()
    for copy in weights[2:6]:
        copy.wait()

    left, right = pl.ds(0, X_FIRST), pl.ds(X_FIRST, Y_FIRST)

    def part_x_copy(plane):
        return send(
            part.at[plane, 1 - x_lo, :, :, left], part_x.at[plane], part_sem, (plane, 0), other_x_lo
        )

    def part_y_copy(plane, step):
        return send(
            part.at[plane, :, y_at(step), :, right],
            part_y.at[plane, step - 1],
            part_sem,
            (plane, step),
            y_device(y_at(step)),
        )

    def mid_x_copy(plane, step):
        return send(
            mid_x.at[plane, y_at(step)],
            fin_x.at[plane, step - 1],
            part_sem,
            (plane, 3 + step),
            y_device(y_at(step)),
        )

    def mid_y_copy(plane):
        return send(mid_y.at[plane], fin_y.at[plane], part_sem, (plane, 7), other_x_lo)

    def project(step):
        plane = around(-offset_of(step))
        core_copy(plane, 1 - core).wait_recv()
        rows = jnp.dot(
            to_strips(), planes[plane].reshape(BLOCK, WIDTH), preferred_element_type=F32
        ).astype(BF16)
        for columns, width in ((left, X_FIRST), (right, Y_FIRST)):
            block = jnp.dot(rows, first[:, columns], preferred_element_type=F32)
            part[plane, :, :, :, columns] = block.astype(BF16).reshape(2, STACK, STRIP, width)
        part_x_copy(plane).start()
        for ahead in range(1, STACK):
            part_y_copy(plane, ahead).start()

        @pl.when(step + 1 < PLANES)
        def _():
            z_landed(step + 1).wait_recv()
            core_copy(around(-offset_of(step + 1)), core).start()

    def halfway(step):
        plane = around(-offset_of(step))
        part_x_copy(plane).wait_recv()
        mid_x[plane] = (
            part[plane, x_lo, :, :, left].astype(F32) + part_x[plane].astype(F32)
        ).astype(BF16)
        for ahead in range(1, STACK):
            mid_x_copy(plane, ahead).start()
        for ahead in range(1, STACK):
            part_y_copy(plane, ahead).wait_recv()

        def total(side):
            parts = [part_y[plane, slot, side].astype(F32) for slot in range(STACK - 1)]
            return part[plane, side, y, :, right].astype(F32) + parts[0] + parts[1] + parts[2]

        mid_y[plane] = total(1 - x_lo).astype(BF16)
        mid_y_copy(plane).start()
        keep_y[plane] = total(x_lo)

    def gelu(inner):
        return (0.5 * inner * (1.0 + lax.erf(inner * math.sqrt(0.5)))).astype(BF16)

    def collect(step):
        plane = around(-offset_of(step))
        for ahead in range(1, STACK):
            mid_x_copy(plane, ahead).wait_recv()
        total = mid_x[plane, y].astype(F32)
        for slot in range(STACK - 1):
            total += fin_x[plane, slot].astype(F32)
        strips[plane] = total[:, : 3 * HEAD].astype(BF16).astype(F32)
        cut = X_FIRST - 3 * HEAD
        acts[plane, x_lo, y, :, HEAD : HEAD + cut] = gelu(total[:, 3 * HEAD :] + bias[:, :cut])
        mid_y_copy(plane).wait_recv()
        total = keep_y[plane] + fin_y[plane].astype(F32)
        acts[plane, x_lo, y, :, HEAD + cut :] = gelu(total + bias[:, cut:])

    bias_copy = weights[6]
    bias_copy.wait()

    def first_half(step, carry):
        @pl.when(step < PLANES)
        def _():
            project(step)

        @pl.when((step >= LAG) & (step < PLANES + LAG))
        def _():
            halfway(step - LAG)

        @pl.when(step >= 2 * LAG)
        def _():
            collect(step - 2 * LAG)

        return carry

    lax.fori_loop(0, PLANES + 2 * LAG, first_half, 0)

    whole = strips[...].reshape(BLOCK, 3 * HEAD)
    query_norm = normalize(whole[:, :HEAD]).astype(BF16)
    key_norm = normalize(whole[:, HEAD : 2 * HEAD]).astype(BF16)
    scores = lax.dot_general(
        query_norm, key_norm, (((1,), (1,)), ((), ())), preferred_element_type=F32
    ) * (temper[...] / math.sqrt(HEAD))
    weight = jnp.exp(scores - jnp.max(scores, axis=-1, keepdims=True))
    probs = (weight / jnp.sum(weight, axis=-1, keepdims=True)).astype(BF16)
    mixed = jnp.dot(probs, whole[:, 2 * HEAD :].astype(BF16), preferred_element_type=F32)
    mixed = mixed.astype(BF16).reshape(PLANES, STRIP, HEAD)
    for plane in range(PLANES):
        acts[plane, x_lo, y, :, :HEAD] = mixed[plane]

    early, late = pl.ds(0, X_ACTS), pl.ds(X_ACTS, SECOND - X_ACTS)

    def acts_x_copy(plane, side):
        place = acts.at[plane, side, y, :, early]
        return send(place, place, acts_sem, (plane, 0), other_x_lo)

    def acts_y_copy(plane, step):
        place = acts.at[plane, x_lo, y]
        return send(place, place, acts_sem, (plane, step), y_device(y_at(step)))

    def acts_y_landed(plane, step):
        place = acts.at[plane, x_lo, y_before(step)]
        return send(place, place, acts_sem, (plane, step), y_device(y_before(step)))

    def pass_y_copy(plane, step):
        place = acts.at[plane, 1 - x_lo, y, :, early]
        return send(place, place, acts_sem, (plane, 3 + step), y_device(y_at(step)))

    def pass_y_landed(plane, step):
        place = acts.at[plane, 1 - x_lo, y_before(step), :, early]
        return send(place, place, acts_sem, (plane, 3 + step), y_device(y_before(step)))

    def pass_x_copy(plane, side):
        place = acts.at[plane, side, :, :, late]
        return send(place, place, acts_sem, (plane, 7), other_x_lo)

    def spread(step):
        plane = around(offset_of(PLANES - 1 - step))
        acts_x_copy(plane, x_lo).start()
        for ahead in range(1, STACK):
            acts_y_copy(plane, ahead).start()

    def pass_on(step):
        plane = around(offset_of(PLANES - 1 - step))
        acts_x_copy(plane, 1 - x_lo).wait_recv()
        for ahead in range(1, STACK):
            pass_y_copy(plane, ahead).start()
        for ahead in range(1, STACK):
            acts_y_landed(plane, ahead).wait_recv()
        pass_x_copy(plane, x_lo).start()

    def pair_copy(plane):
        return send(pair_out.at[plane], pair_in.at[plane], pair_sem, (plane,), other_core)

    def plane_copy(plane, slot):
        return send(plane_out.at[plane], plane_in.at[slot], plane_sem, (slot,), plane_device(plane))

    def plane_landed(slot):
        place = plane_in.at[slot]
        return send(place, place, plane_sem, (slot,), plane_device(around(-offset_of(slot + 1))))

    def output(step):
        plane = around(offset_of(PLANES - 1 - step))
        for ahead in range(1, STACK):
            pass_y_landed(plane, ahead).wait_recv()
        pass_x_copy(plane, 1 - x_lo).wait_recv()
        rows = jnp.dot(
            from_strips(), acts[plane].reshape(BLOCK, SECOND), preferred_element_type=F32
        ).astype(BF16)
        block = jnp.dot(rows, second[...], preferred_element_type=F32).reshape(2, 64, WIDTH)
        pair_out[plane] = jnp.where(core == 0, block[1], block[0]).astype(BF16)
        pair_copy(plane).start()
        pair_own[plane] = jnp.where(core == 0, block[0], block[1])

    def merge(step):
        slot = PLANES - 2 - step
        plane = around(offset_of(slot + 1))
        pair_copy(plane).wait_recv()
        total = pair_own[plane] + pair_in[plane].astype(F32)

        @pl.when(slot >= 0)
        def _():
            plane_out[plane] = total.astype(BF16)
            plane_copy(plane, slot).start()

        @pl.when(slot < 0)
        def _():
            pair_own[plane] = total

    for copy in weights[7:]:
        copy.wait()

    def second_half(step, carry):
        @pl.when(step < PLANES)
        def _():
            spread(step)

        @pl.when((step >= LAG) & (step < PLANES + LAG))
        def _():
            pass_on(step - LAG)

        @pl.when((step >= 2 * LAG) & (step < PLANES + 2 * LAG))
        def _():
            output(step - 2 * LAG)

        @pl.when(step >= 2 * LAG + 1)
        def _():
            merge(step - 2 * LAG - 1)

        return carry

    lax.fori_loop(0, PLANES + 2 * LAG + 1, second_half, 0)
    total = pair_own[z]
    for slot in reversed(range(PLANES - 1)):
        plane_landed(slot).wait_recv()
        total += plane_in[slot].astype(F32)
    lines[...] = total
    for side in range(2):
        for image in range(IMAGES):
            final_out[side, image] = lines[pl.ds(side * 32 + image * ROWS, ROWS), :].astype(BF16)

    def final_copy(step, flip):
        return send(
            final_out.at[half(flip), image_at(step)],
            final_in.at[dp, x_hi],
            final_sem,
            (step, flip),
            (image_at(step), half_mp(flip)),
        )

    def final_landed(step, flip):
        place = final_in.at[image_before(step), half(flip)]
        return send(place, place, final_sem, (step, flip), (image_before(step), half_mp(flip)))

    for piece in pieces:
        final_copy(*piece).start()
    final_in[dp, x_hi] = final_out[x_hi, dp]
    for piece in pieces:
        final_landed(*piece).wait_recv()
    for block in range(IMAGES):
        columns = pl.ds(block * WIDTH, WIDTH)
        total = final_in[block, 0].astype(F32) + final_in[block, 1].astype(F32)
        out[:, columns] = (tokens[:, columns].astype(F32) + total).astype(BF16)

    for piece in pieces:
        norm_copy(*piece).wait_send()
        final_copy(*piece).wait_send()
    for step in range(1, PLANES):
        z_copy(step).wait_send()
        plane_copy(around(offset_of(step)), step - 1).wait_send()

    def sent(plane, carry):
        core_copy(plane, core).wait_send()
        pair_copy(plane).wait_send()
        part_x_copy(plane).wait_send()
        mid_y_copy(plane).wait_send()
        acts_x_copy(plane, x_lo).wait_send()
        pass_x_copy(plane, x_lo).wait_send()
        for ahead in range(1, STACK):
            part_y_copy(plane, ahead).wait_send()
            mid_x_copy(plane, ahead).wait_send()
            acts_y_copy(plane, ahead).wait_send()
            pass_y_copy(plane, ahead).wait_send()
        return carry

    lax.fori_loop(0, PLANES, sent, 0)


def per_device(
    tokens, norm_gain, w_query, w_key, w_value, w_inner, bias_inner, w_attn_out, w_outer, temper
):
    vmem = pl.BlockSpec(memory_space=pltpu.VMEM)
    anywhere = pl.BlockSpec(memory_space=pl.ANY)
    dma = pltpu.SemaphoreType.DMA
    return pl.pallas_call(
        kernel,
        out_shape=jax.ShapeDtypeStruct(tokens.shape, BF16),
        in_specs=[anywhere] * 9 + [vmem],
        out_specs=vmem,
        scratch_shapes=[
            pltpu.VMEM((ROWS, IMAGES * WIDTH), BF16),
            pltpu.VMEM((1, IMAGES * WIDTH), F32),
            pltpu.VMEM((1, HIDDEN), F32),
            pltpu.VMEM((WIDTH, FIRST), BF16),
            pltpu.VMEM((SECOND, WIDTH), BF16),
            pltpu.VMEM((IMAGES, ROWS, WIDTH), BF16),
            pltpu.VMEM((IMAGES, 2, ROWS, WIDTH), BF16),
            pltpu.VMEM((64, WIDTH), F32),
            pltpu.VMEM((PLANES, 2, 64, WIDTH), BF16),
            pltpu.VMEM((PLANES, 2, STACK, STRIP, FIRST), BF16),
            pltpu.VMEM((PLANES, STACK, STRIP, X_FIRST), BF16),
            pltpu.VMEM((PLANES, STACK, STRIP, X_FIRST), BF16),
            pltpu.VMEM((PLANES, STACK - 1, STRIP, X_FIRST), BF16),
            pltpu.VMEM((PLANES, STACK - 1, 2, STRIP, Y_FIRST), BF16),
            pltpu.VMEM((PLANES, STRIP, Y_FIRST), BF16),
            pltpu.VMEM((PLANES, STRIP, Y_FIRST), F32),
            pltpu.VMEM((PLANES, STRIP, Y_FIRST), BF16),
            pltpu.VMEM((PLANES, STRIP, 3 * HEAD), F32),
            pltpu.VMEM((PLANES, 2, STACK, STRIP, SECOND), BF16),
            pltpu.VMEM((PLANES, 64, WIDTH), F32),
            pltpu.VMEM((PLANES, 64, WIDTH), BF16),
            pltpu.VMEM((PLANES, 64, WIDTH), BF16),
            pltpu.VMEM((PLANES, 64, WIDTH), BF16),
            pltpu.VMEM((PLANES - 1, 64, WIDTH), BF16),
            pltpu.VMEM((2, IMAGES, ROWS, WIDTH), BF16),
            pltpu.VMEM((IMAGES, 2, ROWS, WIDTH), BF16),
            dma((9,)),
            dma((2, IMAGES, 2)),
            dma((2, PLANES)),
            dma((2, PLANES)),
            dma((2, PLANES, 8)),
            dma((2, PLANES, 8)),
            dma((2, PLANES)),
            dma((2, PLANES - 1)),
            dma((2, IMAGES, 2)),
        ],
        compiler_params=pltpu.CompilerParams(
            collective_id=0, has_side_effects=True, vmem_limit_bytes=67043328
        ),
    )(
        tokens,
        norm_gain.reshape(1, -1),
        w_query,
        w_key,
        w_value,
        w_inner,
        bias_inner.reshape(1, -1),
        w_attn_out,
        w_outer,
        temper.reshape(1, 1),
    )


def solution(mesh):
    return jax.shard_map(
        per_device,
        mesh=mesh,
        in_specs=(
            P(("dp", "mp"), None),
            P(),
            P("dp", "mp"),
            P("dp", "mp"),
            P("dp", "mp"),
            P("dp", "mp"),
            P("mp"),
            P("mp", "dp"),
            P("mp", "dp"),
            P("mp"),
        ),
        out_specs=P(("dp", "mp"), None),
        check_vma=False,
    )
```

```python
import math

import jax
import jax.numpy as jnp
from jax import lax
from jax.experimental import pallas as pl
from jax.experimental.pallas import tpu as pltpu
from jax.sharding import PartitionSpec as P

HEAD = 128
IMAGES = 8
STACK = 4
PLANES = 8
ROWS = 4
WIDTH = 768
BLOCK = 128
STRIP = 16
HIDDEN = 768
FIRST = 3 * HEAD + HIDDEN
X_FIRST = 640
Y_FIRST = FIRST - X_FIRST
SECOND = HEAD + HIDDEN
LAG = 2
X_ACTS = 512
MESH = pl.DeviceIdType.MESH
F32 = jnp.float32
BF16 = jnp.bfloat16


def offset_of(step):
    return ((step + 1) // 2) * (2 * (step % 2) - 1)


def normalize(values):
    center = values - jnp.mean(values, axis=-1, keepdims=True)
    spread = jnp.mean(center * center, axis=-1, keepdims=True)
    return center * lax.rsqrt(spread + 1e-06)


def gathered_row(place):
    image, within = place >> 4, place & 15
    return ((within >> 2) & 1) * 64 + (within >> 3) * 32 + image * 4 + (within & 3)


def to_strips():
    row = lax.broadcasted_iota(jnp.int32, (BLOCK, BLOCK), 0)
    column = lax.broadcasted_iota(jnp.int32, (BLOCK, BLOCK), 1)
    return jnp.where(column == gathered_row(row), 1.0, 0.0).astype(BF16)


def from_strips():
    row = lax.broadcasted_iota(jnp.int32, (BLOCK, BLOCK), 0)
    column = lax.broadcasted_iota(jnp.int32, (BLOCK, BLOCK), 1)
    return jnp.where(row == gathered_row(column), 1.0, 0.0).astype(BF16)


def kernel(
    tokens_hbm,
    gain_hbm,
    w_query,
    w_key,
    w_value,
    w_inner,
    bias_hbm,
    w_attn_out,
    w_outer,
    temper_hbm,
    out,
    tokens,
    gain,
    bias,
    temper,
    first,
    second,
    norm_out,
    norm_in,
    lines,
    planes,
    part,
    part_x,
    mid_x,
    fin_x,
    part_y,
    mid_y,
    keep_y,
    fin_y,
    strips,
    acts,
    pair_own,
    pair_out,
    pair_in,
    ring_out,
    ring_in,
    final_out,
    final_in,
    w_sem,
    norm_sem,
    z_sem,
    core_sem,
    part_sem,
    acts_sem,
    pair_sem,
    ring_sem,
    final_sem,
):
    dp = lax.axis_index("dp")
    mp = lax.axis_index("mp")
    z, lane = mp // 4, mp % 4
    x_hi, core = lane // 2, lane % 2
    x_lo, y = dp // STACK, dp % STACK
    other_core = (dp, mp + 1 - 2 * core)
    other_x_lo = ((1 - x_lo) * STACK + y, mp)

    def plane_device(plane):
        return (dp, plane * 4 + lane)

    def around(offset):
        return lax.rem(z + offset + PLANES, PLANES)

    def image_at(step):
        return lax.rem(dp + step, IMAGES)

    def image_before(step):
        return lax.rem(dp - step + IMAGES, IMAGES)

    def y_at(step):
        return lax.rem(y + step, STACK)

    def y_before(step):
        return lax.rem(y - step + STACK, STACK)

    def y_device(row):
        return (x_lo * STACK + row, mp)

    def send(source, target, sems, index, device):
        return pltpu.make_async_remote_copy(
            src_ref=source,
            dst_ref=target,
            send_sem=sems.at[(0, *index)],
            recv_sem=sems.at[(1, *index)],
            device_id=device,
            device_id_type=MESH,
        )

    weights = [
        pltpu.make_async_copy(tokens_hbm, tokens, w_sem.at[6]),
        pltpu.make_async_copy(gain_hbm, gain, w_sem.at[7]),
        pltpu.make_async_copy(w_query, first.at[:, pl.ds(0, HEAD)], w_sem.at[0]),
        pltpu.make_async_copy(w_key, first.at[:, pl.ds(HEAD, HEAD)], w_sem.at[1]),
        pltpu.make_async_copy(w_value, first.at[:, pl.ds(2 * HEAD, HEAD)], w_sem.at[2]),
        pltpu.make_async_copy(w_inner, first.at[:, pl.ds(3 * HEAD, HIDDEN)], w_sem.at[3]),
        pltpu.make_async_copy(bias_hbm, bias, w_sem.at[8]),
        pltpu.make_async_copy(temper_hbm, temper, w_sem.at[9]),
        pltpu.make_async_copy(w_attn_out, second.at[pl.ds(0, HEAD), :], w_sem.at[4]),
        pltpu.make_async_copy(w_outer, second.at[pl.ds(HEAD, HIDDEN), :], w_sem.at[5]),
    ]
    for copy in weights[:2]:
        copy.start()
    pieces = [(step, flip) for step in range(IMAGES) for flip in range(2) if step or flip]

    def half(flip):
        return (1 - x_hi) if flip else x_hi

    def half_mp(flip):
        return z * 4 + half(flip) * 2 + core

    barrier = pltpu.get_barrier_semaphore()
    peers = [(image_at(step), half_mp(flip)) for step, flip in pieces]
    peers += [plane_device(around(1)), plane_device(around(-1)), other_core]
    for peer in peers:
        pl.semaphore_signal(barrier, inc=1, device_id=peer, device_id_type=MESH)
    for copy in weights[2:]:
        copy.start()
    for copy in weights[:2]:
        copy.wait()

    normed = (normalize(tokens[...].astype(F32)) * gain[...]).astype(BF16)
    for block in range(IMAGES):
        norm_out[block] = normed[:, block * WIDTH : (block + 1) * WIDTH]
    pl.semaphore_wait(barrier, len(peers))

    def norm_copy(step, flip):
        return send(
            norm_out.at[image_at(step)],
            norm_in.at[dp, x_hi],
            norm_sem,
            (step, flip),
            (image_at(step), half_mp(flip)),
        )

    def norm_landed(step, flip):
        place = norm_in.at[image_before(step), half(flip)]
        return send(place, place, norm_sem, (step, flip), (image_before(step), half_mp(flip)))

    for piece in pieces:
        norm_copy(*piece).start()
    norm_in[dp, x_hi] = norm_out[dp]
    for piece in pieces:
        norm_landed(*piece).wait_recv()
    for side in range(2):
        for image in range(IMAGES):
            lines[pl.ds(side * 32 + image * ROWS, ROWS), :] = norm_in[image, side].astype(F32)
    planes[z, core] = lines[...].astype(BF16)

    def z_way(step):
        return 2 * (step % 2) - 1

    def z_copy(step):
        place = planes.at[around(z_way(step) - offset_of(step)), core]
        return send(place, place, z_sem, (step,), plane_device(around(z_way(step))))

    def z_half_copy(side):
        place = planes.at[around(-3 + 6 * side), core, pl.ds(32 * side, 32)]
        return send(place, place, z_sem, (7 + side,), plane_device(around(1 - 2 * side)))

    def z_landed(step):
        place = planes.at[around(-offset_of(step)), core]
        return send(place, place, z_sem, (step,), plane_device(around(-z_way(step))))

    def z_half_landed(side):
        place = planes.at[around(4), core, pl.ds(32 * side, 32)]
        return send(place, place, z_sem, (7 + side,), plane_device(around(2 * side - 1)))

    def core_copy(plane, side):
        place = planes.at[plane, side]
        return send(place, place, core_sem, (plane,), other_core)

    core_copy(z, core).start()
    for step in (1, 2):
        z_copy(step).start()
    for copy in weights[2:6]:
        copy.wait()

    left, right = pl.ds(0, X_FIRST), pl.ds(X_FIRST, Y_FIRST)

    def part_x_copy(plane):
        return send(
            part.at[plane, 1 - x_lo, :, :, left], part_x.at[plane], part_sem, (plane, 0), other_x_lo
        )

    def part_y_copy(plane, step):
        return send(
            part.at[plane, :, y_at(step), :, right],
            part_y.at[plane, step - 1],
            part_sem,
            (plane, step),
            y_device(y_at(step)),
        )

    def mid_x_copy(plane, step):
        return send(
            mid_x.at[plane, y_at(step)],
            fin_x.at[plane, step - 1],
            part_sem,
            (plane, 3 + step),
            y_device(y_at(step)),
        )

    def mid_y_copy(plane):
        return send(mid_y.at[plane], fin_y.at[plane], part_sem, (plane, 7), other_x_lo)

    def project(step):
        plane = around(-offset_of(step))
        core_copy(plane, 1 - core).wait_recv()
        rows = jnp.dot(
            to_strips(), planes[plane].reshape(BLOCK, WIDTH), preferred_element_type=F32
        ).astype(BF16)
        for columns, width in ((left, X_FIRST), (right, Y_FIRST)):
            block = jnp.dot(rows, first[:, columns], preferred_element_type=F32)
            part[plane, :, :, :, columns] = block.astype(BF16).reshape(2, STACK, STRIP, width)
        part_x_copy(plane).start()
        for ahead in range(1, STACK):
            part_y_copy(plane, ahead).start()

        @pl.when(step + 1 < PLANES)
        def _():
            arrival = step + 1

            @pl.when(arrival < 7)
            def _():
                z_landed(arrival).wait_recv()

            @pl.when(arrival == 7)
            def _():
                for side in range(2):
                    z_half_landed(side).wait_recv()

            @pl.when(arrival < 5)
            def _():
                z_copy(arrival + 2).start()

            for side in range(2):

                @pl.when(arrival == 5 + side)
                def _():
                    z_half_copy(side).start()

            core_copy(around(-offset_of(arrival)), core).start()

    def halfway(step):
        plane = around(-offset_of(step))
        part_x_copy(plane).wait_recv()
        mid_x[plane] = (
            part[plane, x_lo, :, :, left].astype(F32) + part_x[plane].astype(F32)
        ).astype(BF16)
        for ahead in range(1, STACK):
            mid_x_copy(plane, ahead).start()
        for ahead in range(1, STACK):
            part_y_copy(plane, ahead).wait_recv()

        def total(side):
            parts = [part_y[plane, slot, side].astype(F32) for slot in range(STACK - 1)]
            return part[plane, side, y, :, right].astype(F32) + parts[0] + parts[1] + parts[2]

        mid_y[plane] = total(1 - x_lo).astype(BF16)
        mid_y_copy(plane).start()
        keep_y[plane] = total(x_lo)

    def gelu(inner):
        return (0.5 * inner * (1.0 + lax.erf(inner * math.sqrt(0.5)))).astype(BF16)

    def collect(step):
        plane = around(-offset_of(step))
        for ahead in range(1, STACK):
            mid_x_copy(plane, ahead).wait_recv()
        total = mid_x[plane, y].astype(F32)
        for slot in range(STACK - 1):
            total += fin_x[plane, slot].astype(F32)
        strips[plane] = total[:, : 3 * HEAD].astype(BF16).astype(F32)
        cut = X_FIRST - 3 * HEAD
        acts[plane, x_lo, y, :, HEAD : HEAD + cut] = gelu(total[:, 3 * HEAD :] + bias[:cut])
        mid_y_copy(plane).wait_recv()
        total = keep_y[plane] + fin_y[plane].astype(F32)
        acts[plane, x_lo, y, :, HEAD + cut :] = gelu(total + bias[cut:])

    for copy in weights[6:8]:
        copy.wait()

    def first_half(step, carry):
        @pl.when(step < PLANES)
        def _():
            project(step)

        @pl.when((step >= LAG) & (step < PLANES + LAG))
        def _():
            halfway(step - LAG)

        @pl.when(step >= 2 * LAG)
        def _():
            collect(step - 2 * LAG)

        return carry

    lax.fori_loop(0, PLANES + 2 * LAG, first_half, 0)

    whole = strips[...].reshape(BLOCK, 3 * HEAD)
    query_norm = normalize(whole[:, :HEAD]).astype(BF16)
    key_norm = normalize(whole[:, HEAD : 2 * HEAD]).astype(BF16)
    scores = lax.dot_general(
        query_norm, key_norm, (((1,), (1,)), ((), ())), preferred_element_type=F32
    ) * (temper[...].reshape(1, 1) / math.sqrt(HEAD))
    weight = jnp.exp(scores - jnp.max(scores, axis=-1, keepdims=True))
    probs = (weight / jnp.sum(weight, axis=-1, keepdims=True)).astype(BF16)
    mixed = jnp.dot(probs, whole[:, 2 * HEAD :].astype(BF16), preferred_element_type=F32)
    mixed = mixed.astype(BF16).reshape(PLANES, STRIP, HEAD)
    for plane in range(PLANES):
        acts[plane, x_lo, y, :, :HEAD] = mixed[plane]

    early, late = pl.ds(0, X_ACTS), pl.ds(X_ACTS, SECOND - X_ACTS)

    def acts_x_copy(plane, side):
        place = acts.at[plane, side, y, :, early]
        return send(place, place, acts_sem, (plane, 0), other_x_lo)

    def acts_y_copy(plane, step):
        place = acts.at[plane, x_lo, y]
        return send(place, place, acts_sem, (plane, step), y_device(y_at(step)))

    def acts_y_landed(plane, step):
        place = acts.at[plane, x_lo, y_before(step)]
        return send(place, place, acts_sem, (plane, step), y_device(y_before(step)))

    def pass_y_copy(plane, step):
        place = acts.at[plane, 1 - x_lo, y, :, early]
        return send(place, place, acts_sem, (plane, 3 + step), y_device(y_at(step)))

    def pass_y_landed(plane, step):
        place = acts.at[plane, 1 - x_lo, y_before(step), :, early]
        return send(place, place, acts_sem, (plane, 3 + step), y_device(y_before(step)))

    def pass_x_copy(plane, side):
        place = acts.at[plane, side, :, :, late]
        return send(place, place, acts_sem, (plane, 7), other_x_lo)

    def spread(step):
        plane = around(offset_of(PLANES - 1 - step))
        acts_x_copy(plane, x_lo).start()
        for ahead in range(1, STACK):
            acts_y_copy(plane, ahead).start()

    def pass_on(step):
        plane = around(offset_of(PLANES - 1 - step))
        acts_x_copy(plane, 1 - x_lo).wait_recv()
        for ahead in range(1, STACK):
            pass_y_copy(plane, ahead).start()
        for ahead in range(1, STACK):
            acts_y_landed(plane, ahead).wait_recv()
        pass_x_copy(plane, x_lo).start()

    def pair_copy(plane):
        return send(pair_out.at[plane], pair_in.at[plane], pair_sem, (plane,), other_core)

    def ring_copy(step):
        return send(ring_out.at[step], ring_in.at[step], ring_sem, (step,), plane_device(around(-z_way(step))))

    def ring_landed(step):
        return send(ring_in.at[step], ring_in.at[step], ring_sem, (step,), plane_device(around(z_way(step))))

    def ring_half_copy(side):
        rows = pl.ds(32 * side, 32)
        return send(
            ring_out.at[0, rows], ring_in.at[0, rows], ring_sem, (7 * side,), plane_device(around(1 - 2 * side))
        )

    def ring_half_landed(side):
        place = ring_in.at[0, pl.ds(32 * side, 32)]
        return send(place, place, ring_sem, (7 * side,), plane_device(around(2 * side - 1)))

    def output(step):
        plane = around(offset_of(PLANES - 1 - step))
        for ahead in range(1, STACK):
            pass_y_landed(plane, ahead).wait_recv()
        pass_x_copy(plane, 1 - x_lo).wait_recv()
        rows = jnp.dot(
            from_strips(), acts[plane].reshape(BLOCK, SECOND), preferred_element_type=F32
        ).astype(BF16)
        block = jnp.dot(rows, second[...], preferred_element_type=F32).reshape(2, 64, WIDTH)
        pair_out[plane] = jnp.where(core == 0, block[1], block[0]).astype(BF16)
        pair_copy(plane).start()
        pair_own[plane] = jnp.where(core == 0, block[0], block[1])

    def merge(step):
        plane = around(offset_of(PLANES - 1 - step))
        pair_copy(plane).wait_recv()
        pair_own[plane] = pair_own[plane] + pair_in[plane].astype(F32)
        for side in range(2):

            @pl.when(step == 2 - side)
            def _():
                rows = pl.ds(32 * side, 32)
                ring_half_landed(side).wait_recv()
                pair_own[plane, rows] = pair_own[plane, rows] + ring_in[0, rows].astype(F32)

        @pl.when(step >= 3)
        def _():
            ring_landed(step - 2).wait_recv()
            pair_own[plane] = pair_own[plane] + ring_in[step - 2].astype(F32)

        @pl.when(step < PLANES - 1)
        def _():
            ring_out[step] = pair_own[plane].astype(BF16)

        @pl.when(step == 0)
        def _():
            for side in range(2):
                ring_half_copy(side).start()

        @pl.when((step > 0) & (step < PLANES - 1))
        def _():
            ring_copy(step).start()

    for copy in weights[8:]:
        copy.wait()

    def second_half(step, carry):
        @pl.when(step < PLANES)
        def _():
            spread(step)

        @pl.when((step >= LAG) & (step < PLANES + LAG))
        def _():
            pass_on(step - LAG)

        @pl.when((step >= 2 * LAG) & (step < PLANES + 2 * LAG))
        def _():
            output(step - 2 * LAG)

        @pl.when(step >= 2 * LAG + 1)
        def _():
            merge(step - 2 * LAG - 1)

        return carry

    lax.fori_loop(0, PLANES + 2 * LAG + 1, second_half, 0)
    ring_landed(6).wait_recv()
    lines[...] = pair_own[z] + ring_in[6].astype(F32)
    for side in range(2):
        for image in range(IMAGES):
            final_out[side, image] = lines[pl.ds(side * 32 + image * ROWS, ROWS), :].astype(BF16)

    def final_copy(step, flip):
        return send(
            final_out.at[half(flip), image_at(step)],
            final_in.at[dp, x_hi],
            final_sem,
            (step, flip),
            (image_at(step), half_mp(flip)),
        )

    def final_landed(step, flip):
        place = final_in.at[image_before(step), half(flip)]
        return send(place, place, final_sem, (step, flip), (image_before(step), half_mp(flip)))

    for piece in pieces:
        final_copy(*piece).start()
    final_in[dp, x_hi] = final_out[x_hi, dp]
    for piece in pieces:
        final_landed(*piece).wait_recv()
    for block in range(IMAGES):
        columns = pl.ds(block * WIDTH, WIDTH)
        total = final_in[block, 0].astype(F32) + final_in[block, 1].astype(F32)
        out[:, columns] = (tokens[:, columns].astype(F32) + total).astype(BF16)

    for piece in pieces:
        norm_copy(*piece).wait_send()
        final_copy(*piece).wait_send()
    for step in range(1, 7):
        z_copy(step).wait_send()
        ring_copy(step).wait_send()
    for side in range(2):
        z_half_copy(side).wait_send()
        ring_half_copy(side).wait_send()

    def sent(plane, carry):
        core_copy(plane, core).wait_send()
        pair_copy(plane).wait_send()
        part_x_copy(plane).wait_send()
        mid_y_copy(plane).wait_send()
        acts_x_copy(plane, x_lo).wait_send()
        pass_x_copy(plane, x_lo).wait_send()
        for ahead in range(1, STACK):
            part_y_copy(plane, ahead).wait_send()
            mid_x_copy(plane, ahead).wait_send()
            acts_y_copy(plane, ahead).wait_send()
            pass_y_copy(plane, ahead).wait_send()
        return carry

    lax.fori_loop(0, PLANES, sent, 0)


def per_device(
    tokens, norm_gain, w_query, w_key, w_value, w_inner, bias_inner, w_attn_out, w_outer, temper
):
    vmem = pl.BlockSpec(memory_space=pltpu.VMEM)
    hbm = pl.BlockSpec(memory_space=pltpu.HBM)
    dma = pltpu.SemaphoreType.DMA
    return pl.pallas_call(
        kernel,
        out_shape=jax.ShapeDtypeStruct(tokens.shape, BF16),
        in_specs=[hbm] * 10,
        out_specs=vmem,
        scratch_shapes=[
            pltpu.VMEM((ROWS, IMAGES * WIDTH), BF16),
            pltpu.VMEM((1, IMAGES * WIDTH), F32),
            pltpu.VMEM((HIDDEN,), F32),
            pltpu.VMEM((1,), F32),
            pltpu.VMEM((WIDTH, FIRST), BF16),
            pltpu.VMEM((SECOND, WIDTH), BF16),
            pltpu.VMEM((IMAGES, ROWS, WIDTH), BF16),
            pltpu.VMEM((IMAGES, 2, ROWS, WIDTH), BF16),
            pltpu.VMEM((64, WIDTH), F32),
            pltpu.VMEM((PLANES, 2, 64, WIDTH), BF16),
            pltpu.VMEM((PLANES, 2, STACK, STRIP, FIRST), BF16),
            pltpu.VMEM((PLANES, STACK, STRIP, X_FIRST), BF16),
            pltpu.VMEM((PLANES, STACK, STRIP, X_FIRST), BF16),
            pltpu.VMEM((PLANES, STACK - 1, STRIP, X_FIRST), BF16),
            pltpu.VMEM((PLANES, STACK - 1, 2, STRIP, Y_FIRST), BF16),
            pltpu.VMEM((PLANES, STRIP, Y_FIRST), BF16),
            pltpu.VMEM((PLANES, STRIP, Y_FIRST), F32),
            pltpu.VMEM((PLANES, STRIP, Y_FIRST), BF16),
            pltpu.VMEM((PLANES, STRIP, 3 * HEAD), F32),
            pltpu.VMEM((PLANES, 2, STACK, STRIP, SECOND), BF16),
            pltpu.VMEM((PLANES, 64, WIDTH), F32),
            pltpu.VMEM((PLANES, 64, WIDTH), BF16),
            pltpu.VMEM((PLANES, 64, WIDTH), BF16),
            pltpu.VMEM((PLANES - 1, 64, WIDTH), BF16),
            pltpu.VMEM((PLANES - 1, 64, WIDTH), BF16),
            pltpu.VMEM((2, IMAGES, ROWS, WIDTH), BF16),
            pltpu.VMEM((IMAGES, 2, ROWS, WIDTH), BF16),
            dma((10,)),
            dma((2, IMAGES, 2)),
            dma((2, 9)),
            dma((2, PLANES)),
            dma((2, PLANES, 8)),
            dma((2, PLANES, 8)),
            dma((2, PLANES)),
            dma((2, PLANES)),
            dma((2, IMAGES, 2)),
        ],
        compiler_params=pltpu.CompilerParams(
            collective_id=0, has_side_effects=True, vmem_limit_bytes=67043328
        ),
    )(
        tokens,
        norm_gain.reshape(1, -1),
        w_query,
        w_key,
        w_value,
        w_inner,
        bias_inner,
        w_attn_out,
        w_outer,
        temper,
    )


def solution(mesh):
    return jax.shard_map(
        per_device,
        mesh=mesh,
        in_specs=(
            P(("dp", "mp"), None),
            P(),
            P("dp", "mp"),
            P("dp", "mp"),
            P("dp", "mp"),
            P("dp", "mp"),
            P("mp"),
            P("mp", "dp"),
            P("mp", "dp"),
            P("mp"),
        ),
        out_specs=P(("dp", "mp"), None),
        check_vma=False,
    )
```

```python
import math

import jax
import jax.numpy as jnp
from jax import lax
from jax.experimental import pallas as pl
from jax.experimental.pallas import tpu as pltpu
from jax.sharding import PartitionSpec as P

HEAD = 128
IMAGES = 8
STACK = 4
PLANES = 8
ROWS = 4
WIDTH = 768
BLOCK = 128
STRIP = 16
HIDDEN = 768
FIRST = 3 * HEAD + HIDDEN
X_FIRST = 640
Y_FIRST = FIRST - X_FIRST
SECOND = HEAD + HIDDEN
LAG = 2
X_ACTS = 384
AHEAD = 3
MESH = pl.DeviceIdType.MESH
F32 = jnp.float32
BF16 = jnp.bfloat16


def offset_of(step):
    return ((step + 1) // 2) * (2 * (step % 2) - 1)


def normalize(values):
    center = values - jnp.mean(values, axis=-1, keepdims=True)
    spread = jnp.mean(center * center, axis=-1, keepdims=True)
    return center * lax.rsqrt(spread + 1e-06)


def gathered_row(place):
    image, within = place >> 4, place & 15
    return ((within >> 2) & 1) * 64 + (within >> 3) * 32 + image * 4 + (within & 3)


def to_strips():
    row = lax.broadcasted_iota(jnp.int32, (BLOCK, BLOCK), 0)
    column = lax.broadcasted_iota(jnp.int32, (BLOCK, BLOCK), 1)
    return jnp.where(column == gathered_row(row), 1.0, 0.0).astype(BF16)


def from_strips():
    row = lax.broadcasted_iota(jnp.int32, (BLOCK, BLOCK), 0)
    column = lax.broadcasted_iota(jnp.int32, (BLOCK, BLOCK), 1)
    return jnp.where(row == gathered_row(column), 1.0, 0.0).astype(BF16)


def kernel(
    tokens_hbm,
    gain_hbm,
    w_query,
    w_key,
    w_value,
    w_inner,
    bias_hbm,
    w_attn_out,
    w_outer,
    temper_hbm,
    out,
    tokens,
    gain,
    bias,
    temper,
    first,
    second,
    norm_out,
    norm_in,
    lines,
    planes,
    part,
    part_x,
    mid_x,
    fin_x,
    part_y,
    mid_y,
    keep_y,
    fin_y,
    strips,
    acts,
    pair_own,
    pair_out,
    pair_in,
    ring_out,
    ring_in,
    final_out,
    final_in,
    w_sem,
    norm_sem,
    z_sem,
    core_sem,
    part_sem,
    acts_sem,
    mixed_sem,
    pair_sem,
    ring_sem,
    final_sem,
):
    dp = lax.axis_index("dp")
    mp = lax.axis_index("mp")
    z, lane = mp // 4, mp % 4
    x_hi, core = lane // 2, lane % 2
    x_lo, y = dp // STACK, dp % STACK
    other_core = (dp, mp + 1 - 2 * core)
    other_x_lo = ((1 - x_lo) * STACK + y, mp)

    def plane_device(plane):
        return (dp, plane * 4 + lane)

    def around(offset):
        return lax.rem(z + offset + PLANES, PLANES)

    def image_at(step):
        return lax.rem(dp + step, IMAGES)

    def image_before(step):
        return lax.rem(dp - step + IMAGES, IMAGES)

    def y_at(step):
        return lax.rem(y + step, STACK)

    def y_before(step):
        return lax.rem(y - step + STACK, STACK)

    def y_device(row):
        return (x_lo * STACK + row, mp)

    def send(source, target, sems, index, device):
        return pltpu.make_async_remote_copy(
            src_ref=source,
            dst_ref=target,
            send_sem=sems.at[(0, *index)],
            recv_sem=sems.at[(1, *index)],
            device_id=device,
            device_id_type=MESH,
        )

    weights = [
        pltpu.make_async_copy(tokens_hbm, tokens, w_sem.at[6]),
        pltpu.make_async_copy(gain_hbm, gain, w_sem.at[7]),
        pltpu.make_async_copy(w_query, first.at[:, pl.ds(0, HEAD)], w_sem.at[0]),
        pltpu.make_async_copy(w_key, first.at[:, pl.ds(HEAD, HEAD)], w_sem.at[1]),
        pltpu.make_async_copy(w_value, first.at[:, pl.ds(2 * HEAD, HEAD)], w_sem.at[2]),
        pltpu.make_async_copy(w_inner, first.at[:, pl.ds(3 * HEAD, HIDDEN)], w_sem.at[3]),
        pltpu.make_async_copy(bias_hbm, bias, w_sem.at[8]),
        pltpu.make_async_copy(temper_hbm, temper, w_sem.at[9]),
        pltpu.make_async_copy(w_attn_out, second.at[pl.ds(0, HEAD), :], w_sem.at[4]),
        pltpu.make_async_copy(w_outer, second.at[pl.ds(HEAD, HIDDEN), :], w_sem.at[5]),
    ]
    for copy in weights[:2]:
        copy.start()
    pieces = [(step, flip) for step in range(IMAGES) for flip in range(2) if step or flip]

    def half(flip):
        return (1 - x_hi) if flip else x_hi

    def half_mp(flip):
        return z * 4 + half(flip) * 2 + core

    barrier = pltpu.get_barrier_semaphore()
    peers = [(image_at(step), half_mp(flip)) for step, flip in pieces]
    peers += [plane_device(around(1)), plane_device(around(-1)), other_core]
    for peer in peers:
        pl.semaphore_signal(barrier, inc=1, device_id=peer, device_id_type=MESH)
    for copy in weights[2:]:
        copy.start()
    for copy in weights[:2]:
        copy.wait()

    normed = (normalize(tokens[...].astype(F32)) * gain[...]).astype(BF16)
    for block in range(IMAGES):
        norm_out[block] = normed[:, block * WIDTH : (block + 1) * WIDTH]
    pl.semaphore_wait(barrier, len(peers))

    def norm_copy(step, flip):
        return send(
            norm_out.at[image_at(step)],
            norm_in.at[dp, x_hi],
            norm_sem,
            (step, flip),
            (image_at(step), half_mp(flip)),
        )

    def norm_landed(step, flip):
        place = norm_in.at[image_before(step), half(flip)]
        return send(place, place, norm_sem, (step, flip), (image_before(step), half_mp(flip)))

    for piece in pieces:
        norm_copy(*piece).start()
    norm_in[dp, x_hi] = norm_out[dp]
    for piece in pieces:
        norm_landed(*piece).wait_recv()
    for side in range(2):
        for image in range(IMAGES):
            lines[pl.ds(side * 32 + image * ROWS, ROWS), :] = norm_in[image, side].astype(F32)
    planes[z, core] = lines[...].astype(BF16)

    def z_way(step):
        return 2 * (step % 2) - 1

    def z_copy(step):
        place = planes.at[around(z_way(step) - offset_of(step)), core]
        return send(place, place, z_sem, (step,), plane_device(around(z_way(step))))

    def z_half_copy(side):
        place = planes.at[around(-3 + 6 * side), core, pl.ds(32 * side, 32)]
        return send(place, place, z_sem, (7 + side,), plane_device(around(1 - 2 * side)))

    def z_landed(step):
        place = planes.at[around(-offset_of(step)), core]
        return send(place, place, z_sem, (step,), plane_device(around(-z_way(step))))

    def z_half_landed(side):
        place = planes.at[around(4), core, pl.ds(32 * side, 32)]
        return send(place, place, z_sem, (7 + side,), plane_device(around(2 * side - 1)))

    def core_copy(plane, side):
        place = planes.at[plane, side]
        return send(place, place, core_sem, (plane,), other_core)

    core_copy(z, core).start()
    for step in (1, 2):
        z_copy(step).start()
    for copy in weights[2:6]:
        copy.wait()

    left, right = pl.ds(0, X_FIRST), pl.ds(X_FIRST, Y_FIRST)

    def part_x_copy(plane):
        return send(
            part.at[plane, 1 - x_lo, :, :, left], part_x.at[plane], part_sem, (plane, 0), other_x_lo
        )

    def part_y_copy(plane, step):
        return send(
            part.at[plane, :, y_at(step), :, right],
            part_y.at[plane, step - 1],
            part_sem,
            (plane, step),
            y_device(y_at(step)),
        )

    def mid_x_copy(plane, step):
        return send(
            mid_x.at[plane, y_at(step)],
            fin_x.at[plane, step - 1],
            part_sem,
            (plane, 3 + step),
            y_device(y_at(step)),
        )

    def mid_y_copy(plane):
        return send(mid_y.at[plane], fin_y.at[plane], part_sem, (plane, 7), other_x_lo)

    def project(step):
        plane = around(-offset_of(step))
        core_copy(plane, 1 - core).wait_recv()
        rows = jnp.dot(
            to_strips(), planes[plane].reshape(BLOCK, WIDTH), preferred_element_type=F32
        ).astype(BF16)
        for columns, width in ((left, X_FIRST), (right, Y_FIRST)):
            block = jnp.dot(rows, first[:, columns], preferred_element_type=F32)
            part[plane, :, :, :, columns] = block.astype(BF16).reshape(2, STACK, STRIP, width)
        part_x_copy(plane).start()
        for ahead in range(1, STACK):
            part_y_copy(plane, ahead).start()

        @pl.when(step + 1 < PLANES)
        def _():
            arrival = step + 1

            @pl.when(arrival < 7)
            def _():
                z_landed(arrival).wait_recv()

            @pl.when(arrival == 7)
            def _():
                for side in range(2):
                    z_half_landed(side).wait_recv()

            @pl.when(arrival < 5)
            def _():
                z_copy(arrival + 2).start()

            for side in range(2):

                @pl.when(arrival == 5 + side)
                def _():
                    z_half_copy(side).start()

            core_copy(around(-offset_of(arrival)), core).start()

    def halfway(step):
        plane = around(-offset_of(step))
        part_x_copy(plane).wait_recv()
        mid_x[plane] = (
            part[plane, x_lo, :, :, left].astype(F32) + part_x[plane].astype(F32)
        ).astype(BF16)
        for ahead in range(1, STACK):
            mid_x_copy(plane, ahead).start()
        for ahead in range(1, STACK):
            part_y_copy(plane, ahead).wait_recv()

        def total(side):
            parts = [part_y[plane, slot, side].astype(F32) for slot in range(STACK - 1)]
            return part[plane, side, y, :, right].astype(F32) + parts[0] + parts[1] + parts[2]

        mid_y[plane] = total(1 - x_lo).astype(BF16)
        mid_y_copy(plane).start()
        keep_y[plane] = total(x_lo)

    def gelu(inner):
        return (0.5 * inner * (1.0 + lax.erf(inner * math.sqrt(0.5)))).astype(BF16)

    def collect(step):
        plane = around(-offset_of(step))
        for ahead in range(1, STACK):
            mid_x_copy(plane, ahead).wait_recv()
        total = mid_x[plane, y].astype(F32)
        for slot in range(STACK - 1):
            total += fin_x[plane, slot].astype(F32)
        strips[plane] = total[:, : 3 * HEAD].astype(BF16).astype(F32)
        cut = X_FIRST - 3 * HEAD
        acts[plane, x_lo, y, :, HEAD : HEAD + cut] = gelu(total[:, 3 * HEAD :] + bias[:cut])
        mid_y_copy(plane).wait_recv()
        total = keep_y[plane] + fin_y[plane].astype(F32)
        acts[plane, x_lo, y, :, HEAD + cut :] = gelu(total + bias[cut:])

    for copy in weights[6:8]:
        copy.wait()

    hidden = pl.ds(HEAD, HIDDEN)
    early, late = pl.ds(HEAD, X_ACTS), pl.ds(HEAD + X_ACTS, HIDDEN - X_ACTS)

    def mixed_copy(step):
        place = acts.at[:, x_lo, y, :, pl.ds(0, HEAD)]
        return send(place, place, mixed_sem, (step,), (image_at(step), mp))

    def mixed_landed(step):
        image = image_before(step)
        place = acts.at[:, image // STACK, image % STACK, :, pl.ds(0, HEAD)]
        return send(place, place, mixed_sem, (step,), (image, mp))

    def acts_x_copy(plane, side):
        place = acts.at[plane, side, y, :, early]
        return send(place, place, acts_sem, (plane, 0), other_x_lo)

    def acts_y_copy(plane, step):
        place = acts.at[plane, x_lo, y, :, hidden]
        return send(place, place, acts_sem, (plane, step), y_device(y_at(step)))

    def acts_y_landed(plane, step):
        place = acts.at[plane, x_lo, y_before(step), :, hidden]
        return send(place, place, acts_sem, (plane, step), y_device(y_before(step)))

    def pass_y_copy(plane, step):
        place = acts.at[plane, 1 - x_lo, y, :, early]
        return send(place, place, acts_sem, (plane, 3 + step), y_device(y_at(step)))

    def pass_y_landed(plane, step):
        place = acts.at[plane, 1 - x_lo, y_before(step), :, early]
        return send(place, place, acts_sem, (plane, 3 + step), y_device(y_before(step)))

    def pass_x_copy(plane, side):
        place = acts.at[plane, side, :, :, late]
        return send(place, place, acts_sem, (plane, 7), other_x_lo)

    def spread(step):
        plane = around(offset_of(PLANES - 1 - step))
        acts_x_copy(plane, x_lo).start()
        for ahead in range(1, STACK):
            acts_y_copy(plane, ahead).start()

    def pass_on(step):
        plane = around(offset_of(PLANES - 1 - step))
        acts_x_copy(plane, 1 - x_lo).wait_recv()
        for ahead in range(1, STACK):
            pass_y_copy(plane, ahead).start()
        for ahead in range(1, STACK):
            acts_y_landed(plane, ahead).wait_recv()
        pass_x_copy(plane, x_lo).start()

    def first_half(step, carry):
        @pl.when((step >= LAG) & (step < PLANES + LAG))
        def _():
            halfway(step - LAG)

        @pl.when(step == PLANES + LAG - 1)
        def _():
            for behind in range(AHEAD):
                spread(PLANES - 1 - behind)

        @pl.when(step < PLANES)
        def _():
            project(step)

        @pl.when(step >= 2 * LAG)
        def _():
            collect(step - 2 * LAG)

        return carry

    lax.fori_loop(0, PLANES + 2 * LAG, first_half, 0)

    whole = strips[...].reshape(BLOCK, 3 * HEAD)
    query_norm = normalize(whole[:, :HEAD]).astype(BF16)
    key_norm = normalize(whole[:, HEAD : 2 * HEAD]).astype(BF16)
    scores = lax.dot_general(
        query_norm, key_norm, (((1,), (1,)), ((), ())), preferred_element_type=F32
    ) * (temper[...].reshape(1, 1) / math.sqrt(HEAD))
    weight = jnp.exp(scores - jnp.max(scores, axis=-1, keepdims=True))
    probs = (weight / jnp.sum(weight, axis=-1, keepdims=True)).astype(BF16)
    mixed = jnp.dot(probs, whole[:, 2 * HEAD :].astype(BF16), preferred_element_type=F32)
    mixed = mixed.astype(BF16).reshape(PLANES, STRIP, HEAD)
    for plane in range(PLANES):
        acts[plane, x_lo, y, :, :HEAD] = mixed[plane]
    for step in range(1, IMAGES):
        mixed_copy(step).start()

    def pair_copy(plane):
        return send(pair_out.at[plane], pair_in.at[plane], pair_sem, (plane,), other_core)

    def ring_copy(step):
        return send(ring_out.at[step], ring_in.at[step], ring_sem, (step,), plane_device(around(-z_way(step))))

    def ring_landed(step):
        return send(ring_in.at[step], ring_in.at[step], ring_sem, (step,), plane_device(around(z_way(step))))

    def ring_half_copy(side):
        rows = pl.ds(32 * side, 32)
        return send(
            ring_out.at[0, rows], ring_in.at[0, rows], ring_sem, (7 * side,), plane_device(around(1 - 2 * side))
        )

    def ring_half_landed(side):
        place = ring_in.at[0, pl.ds(32 * side, 32)]
        return send(place, place, ring_sem, (7 * side,), plane_device(around(2 * side - 1)))

    def output(step):
        plane = around(offset_of(PLANES - 1 - step))
        for ahead in range(1, STACK):
            pass_y_landed(plane, ahead).wait_recv()
        pass_x_copy(plane, 1 - x_lo).wait_recv()
        rows = jnp.dot(
            from_strips(), acts[plane].reshape(BLOCK, SECOND), preferred_element_type=F32
        ).astype(BF16)
        block = jnp.dot(rows, second[...], preferred_element_type=F32).reshape(2, 64, WIDTH)
        pair_out[plane] = jnp.where(core == 0, block[1], block[0]).astype(BF16)
        pair_copy(plane).start()
        pair_own[plane] = jnp.where(core == 0, block[0], block[1])

    def merge(step):
        plane = around(offset_of(PLANES - 1 - step))
        pair_copy(plane).wait_recv()
        pair_own[plane] = pair_own[plane] + pair_in[plane].astype(F32)
        for side in range(2):

            @pl.when(step == 2 - side)
            def _():
                rows = pl.ds(32 * side, 32)
                ring_half_landed(side).wait_recv()
                pair_own[plane, rows] = pair_own[plane, rows] + ring_in[0, rows].astype(F32)

        @pl.when(step >= 3)
        def _():
            ring_landed(step - 2).wait_recv()
            pair_own[plane] = pair_own[plane] + ring_in[step - 2].astype(F32)

        @pl.when(step < PLANES - 1)
        def _():
            ring_out[step] = pair_own[plane].astype(BF16)

        @pl.when(step == 0)
        def _():
            for side in range(2):
                ring_half_copy(side).start()

        @pl.when((step > 0) & (step < PLANES - 1))
        def _():
            ring_copy(step).start()

    for copy in weights[8:]:
        copy.wait()

    def second_half(step, carry):
        @pl.when(step < PLANES - AHEAD)
        def _():
            spread(step)

        @pl.when(step < AHEAD)
        def _():
            pass_on(PLANES - AHEAD + step)

        @pl.when((step >= LAG) & (step < PLANES - AHEAD + LAG))
        def _():
            pass_on(step - LAG)

        @pl.when(step == 2 * LAG)
        def _():
            for ahead in range(1, IMAGES):
                mixed_landed(ahead).wait_recv()

        @pl.when(step >= 2 * LAG + 1)
        def _():
            merge(step - 2 * LAG - 1)

        @pl.when((step >= 2 * LAG) & (step < PLANES + 2 * LAG))
        def _():
            output(step - 2 * LAG)

        return carry

    lax.fori_loop(0, PLANES + 2 * LAG + 1, second_half, 0)
    ring_landed(6).wait_recv()
    lines[...] = pair_own[z] + ring_in[6].astype(F32)
    for side in range(2):
        for image in range(IMAGES):
            final_out[side, image] = lines[pl.ds(side * 32 + image * ROWS, ROWS), :].astype(BF16)

    def final_copy(step, flip):
        return send(
            final_out.at[half(flip), image_at(step)],
            final_in.at[dp, x_hi],
            final_sem,
            (step, flip),
            (image_at(step), half_mp(flip)),
        )

    def final_landed(step, flip):
        place = final_in.at[image_before(step), half(flip)]
        return send(place, place, final_sem, (step, flip), (image_before(step), half_mp(flip)))

    for piece in pieces:
        final_copy(*piece).start()
    final_in[dp, x_hi] = final_out[x_hi, dp]
    for piece in pieces:
        final_landed(*piece).wait_recv()
    for block in range(IMAGES):
        columns = pl.ds(block * WIDTH, WIDTH)
        total = final_in[block, 0].astype(F32) + final_in[block, 1].astype(F32)
        out[:, columns] = (tokens[:, columns].astype(F32) + total).astype(BF16)

    for step in range(1, IMAGES):
        mixed_copy(step).wait_send()
    for piece in pieces:
        norm_copy(*piece).wait_send()
        final_copy(*piece).wait_send()
    for step in range(1, 7):
        z_copy(step).wait_send()
        ring_copy(step).wait_send()
    for side in range(2):
        z_half_copy(side).wait_send()
        ring_half_copy(side).wait_send()

    def sent(plane, carry):
        core_copy(plane, core).wait_send()
        pair_copy(plane).wait_send()
        part_x_copy(plane).wait_send()
        mid_y_copy(plane).wait_send()
        acts_x_copy(plane, x_lo).wait_send()
        pass_x_copy(plane, x_lo).wait_send()
        for ahead in range(1, STACK):
            part_y_copy(plane, ahead).wait_send()
            mid_x_copy(plane, ahead).wait_send()
            acts_y_copy(plane, ahead).wait_send()
            pass_y_copy(plane, ahead).wait_send()
        return carry

    lax.fori_loop(0, PLANES, sent, 0)


def per_device(
    tokens, norm_gain, w_query, w_key, w_value, w_inner, bias_inner, w_attn_out, w_outer, temper
):
    vmem = pl.BlockSpec(memory_space=pltpu.VMEM)
    hbm = pl.BlockSpec(memory_space=pltpu.HBM)
    dma = pltpu.SemaphoreType.DMA
    return pl.pallas_call(
        kernel,
        out_shape=jax.ShapeDtypeStruct(tokens.shape, BF16),
        in_specs=[hbm] * 10,
        out_specs=vmem,
        scratch_shapes=[
            pltpu.VMEM((ROWS, IMAGES * WIDTH), BF16),
            pltpu.VMEM((1, IMAGES * WIDTH), F32),
            pltpu.VMEM((HIDDEN,), F32),
            pltpu.VMEM((1,), F32),
            pltpu.VMEM((WIDTH, FIRST), BF16),
            pltpu.VMEM((SECOND, WIDTH), BF16),
            pltpu.VMEM((IMAGES, ROWS, WIDTH), BF16),
            pltpu.VMEM((IMAGES, 2, ROWS, WIDTH), BF16),
            pltpu.VMEM((64, WIDTH), F32),
            pltpu.VMEM((PLANES, 2, 64, WIDTH), BF16),
            pltpu.VMEM((PLANES, 2, STACK, STRIP, FIRST), BF16),
            pltpu.VMEM((PLANES, STACK, STRIP, X_FIRST), BF16),
            pltpu.VMEM((PLANES, STACK, STRIP, X_FIRST), BF16),
            pltpu.VMEM((PLANES, STACK - 1, STRIP, X_FIRST), BF16),
            pltpu.VMEM((PLANES, STACK - 1, 2, STRIP, Y_FIRST), BF16),
            pltpu.VMEM((PLANES, STRIP, Y_FIRST), BF16),
            pltpu.VMEM((PLANES, STRIP, Y_FIRST), F32),
            pltpu.VMEM((PLANES, STRIP, Y_FIRST), BF16),
            pltpu.VMEM((PLANES, STRIP, 3 * HEAD), F32),
            pltpu.VMEM((PLANES, 2, STACK, STRIP, SECOND), BF16),
            pltpu.VMEM((PLANES, 64, WIDTH), F32),
            pltpu.VMEM((PLANES, 64, WIDTH), BF16),
            pltpu.VMEM((PLANES, 64, WIDTH), BF16),
            pltpu.VMEM((PLANES - 1, 64, WIDTH), BF16),
            pltpu.VMEM((PLANES - 1, 64, WIDTH), BF16),
            pltpu.VMEM((2, IMAGES, ROWS, WIDTH), BF16),
            pltpu.VMEM((IMAGES, 2, ROWS, WIDTH), BF16),
            dma((10,)),
            dma((2, IMAGES, 2)),
            dma((2, 9)),
            dma((2, PLANES)),
            dma((2, PLANES, 8)),
            dma((2, PLANES, 8)),
            dma((2, IMAGES)),
            dma((2, PLANES)),
            dma((2, PLANES)),
            dma((2, IMAGES, 2)),
        ],
        compiler_params=pltpu.CompilerParams(
            collective_id=0, has_side_effects=True, vmem_limit_bytes=67043328
        ),
    )(
        tokens,
        norm_gain.reshape(1, -1),
        w_query,
        w_key,
        w_value,
        w_inner,
        bias_inner,
        w_attn_out,
        w_outer,
        temper,
    )


def solution(mesh):
    return jax.shard_map(
        per_device,
        mesh=mesh,
        in_specs=(
            P(("dp", "mp"), None),
            P(),
            P("dp", "mp"),
            P("dp", "mp"),
            P("dp", "mp"),
            P("dp", "mp"),
            P("mp"),
            P("mp", "dp"),
            P("mp", "dp"),
            P("mp"),
        ),
        out_specs=P(("dp", "mp"), None),
        check_vma=False,
    )
```

```python
import math

import jax
import jax.numpy as jnp
from jax import lax
from jax.experimental import pallas as pl
from jax.experimental.pallas import tpu as pltpu
from jax.sharding import PartitionSpec as P

HEAD = 128
IMAGES = 8
STACK = 4
PLANES = 8
ROWS = 4
WIDTH = 768
BLOCK = 128
STRIP = 16
HIDDEN = 768
FIRST = 3 * HEAD + HIDDEN
X_FIRST = 640
Y_FIRST = FIRST - X_FIRST
SECOND = HEAD + HIDDEN
LAG = 2
X_ACTS = 384
STRAIGHT = 2
STAGED = PLANES - STRAIGHT
AHEAD = 0
SOON = 2
FAR_FIRST = (2, 1, 3)
MESH = pl.DeviceIdType.MESH
F32 = jnp.float32
BF16 = jnp.bfloat16


def offset_of(step):
    return ((step + 1) // 2) * (2 * (step % 2) - 1)


def normalize(values):
    center = values - jnp.mean(values, axis=-1, keepdims=True)
    spread = jnp.mean(center * center, axis=-1, keepdims=True)
    return center * lax.rsqrt(spread + 1e-06)


def gathered_row(place):
    image, within = place >> 4, place & 15
    return ((within >> 2) & 1) * 64 + (within >> 3) * 32 + image * 4 + (within & 3)


def to_strips():
    row = lax.broadcasted_iota(jnp.int32, (BLOCK, BLOCK), 0)
    column = lax.broadcasted_iota(jnp.int32, (BLOCK, BLOCK), 1)
    return jnp.where(column == gathered_row(row), 1.0, 0.0).astype(BF16)


def from_strips():
    row = lax.broadcasted_iota(jnp.int32, (BLOCK, BLOCK), 0)
    column = lax.broadcasted_iota(jnp.int32, (BLOCK, BLOCK), 1)
    return jnp.where(row == gathered_row(column), 1.0, 0.0).astype(BF16)


def kernel(
    tokens_hbm,
    gain_hbm,
    w_query,
    w_key,
    w_value,
    w_inner,
    bias_hbm,
    w_attn_out,
    w_outer,
    temper_hbm,
    out,
    tokens,
    gain,
    bias,
    temper,
    first,
    second,
    norm_out,
    norm_in,
    lines,
    planes,
    part,
    part_x,
    mid_x,
    fin_x,
    part_y,
    mid_y,
    keep_y,
    fin_y,
    straight_in,
    strips,
    acts,
    pair_own,
    pair_out,
    pair_in,
    ring_out,
    ring_in,
    final_out,
    final_in,
    w_sem,
    norm_sem,
    z_sem,
    core_sem,
    part_sem,
    straight_sem,
    acts_sem,
    mixed_sem,
    pair_sem,
    ring_sem,
    final_sem,
):
    dp = lax.axis_index("dp")
    mp = lax.axis_index("mp")
    z, lane = mp // 4, mp % 4
    x_hi, core = lane // 2, lane % 2
    x_lo, y = dp // STACK, dp % STACK
    other_core = (dp, mp + 1 - 2 * core)
    other_x_lo = ((1 - x_lo) * STACK + y, mp)

    def plane_device(plane):
        return (dp, plane * 4 + lane)

    def around(offset):
        return lax.rem(z + offset + PLANES, PLANES)

    def image_at(step):
        return lax.rem(dp + step, IMAGES)

    def image_before(step):
        return lax.rem(dp - step + IMAGES, IMAGES)

    def y_at(step):
        return lax.rem(y + step, STACK)

    def y_before(step):
        return lax.rem(y - step + STACK, STACK)

    def y_device(row):
        return (x_lo * STACK + row, mp)

    def send(source, target, sems, index, device):
        return pltpu.make_async_remote_copy(
            src_ref=source,
            dst_ref=target,
            send_sem=sems.at[(0, *index)],
            recv_sem=sems.at[(1, *index)],
            device_id=device,
            device_id_type=MESH,
        )

    weights = [
        pltpu.make_async_copy(tokens_hbm, tokens, w_sem.at[6]),
        pltpu.make_async_copy(gain_hbm, gain, w_sem.at[7]),
        pltpu.make_async_copy(w_query, first.at[:, pl.ds(0, HEAD)], w_sem.at[0]),
        pltpu.make_async_copy(w_key, first.at[:, pl.ds(HEAD, HEAD)], w_sem.at[1]),
        pltpu.make_async_copy(w_value, first.at[:, pl.ds(2 * HEAD, HEAD)], w_sem.at[2]),
        pltpu.make_async_copy(w_inner, first.at[:, pl.ds(3 * HEAD, HIDDEN)], w_sem.at[3]),
        pltpu.make_async_copy(bias_hbm, bias, w_sem.at[8]),
        pltpu.make_async_copy(temper_hbm, temper, w_sem.at[9]),
        pltpu.make_async_copy(w_attn_out, second.at[pl.ds(0, HEAD), :], w_sem.at[4]),
        pltpu.make_async_copy(w_outer, second.at[pl.ds(HEAD, HIDDEN), :], w_sem.at[5]),
    ]
    for copy in weights[:2]:
        copy.start()
    pieces = [(step, flip) for step in range(IMAGES) for flip in range(2) if step or flip]

    def half(flip):
        return (1 - x_hi) if flip else x_hi

    def half_mp(flip):
        return z * 4 + half(flip) * 2 + core

    barrier = pltpu.get_barrier_semaphore()
    peers = [(image_at(step), half_mp(flip)) for step, flip in pieces]
    peers += [plane_device(around(offset)) for offset in (1, -1)] + [other_core]
    for peer in peers:
        pl.semaphore_signal(barrier, inc=1, device_id=peer, device_id_type=MESH)
    for copy in weights[2:]:
        copy.start()
    for copy in weights[:2]:
        copy.wait()

    normed = (normalize(tokens[...].astype(F32)) * gain[...]).astype(BF16)
    for block in range(IMAGES):
        norm_out[block] = normed[:, block * WIDTH : (block + 1) * WIDTH]
    pl.semaphore_wait(barrier, len(peers))

    def norm_copy(step, flip):
        return send(
            norm_out.at[image_at(step)],
            norm_in.at[dp, x_hi],
            norm_sem,
            (step, flip),
            (image_at(step), half_mp(flip)),
        )

    def norm_landed(step, flip):
        place = norm_in.at[image_before(step), half(flip)]
        return send(place, place, norm_sem, (step, flip), (image_before(step), half_mp(flip)))

    for piece in pieces:
        norm_copy(*piece).start()
    norm_in[dp, x_hi] = norm_out[dp]
    for piece in pieces:
        norm_landed(*piece).wait_recv()
    for side in range(2):
        for image in range(IMAGES):
            lines[pl.ds(side * 32 + image * ROWS, ROWS), :] = norm_in[image, side].astype(F32)
    planes[z, core] = lines[...].astype(BF16)

    def z_way(step):
        return 2 * (step % 2) - 1

    def z_copy(step):
        place = planes.at[around(z_way(step) - offset_of(step)), core]
        return send(place, place, z_sem, (step,), plane_device(around(z_way(step))))

    def z_half_copy(side):
        place = planes.at[around(-3 + 6 * side), core, pl.ds(32 * side, 32)]
        return send(place, place, z_sem, (7 + side,), plane_device(around(1 - 2 * side)))

    def z_landed(step):
        place = planes.at[around(-offset_of(step)), core]
        return send(place, place, z_sem, (step,), plane_device(around(-z_way(step))))

    def z_half_landed(side):
        place = planes.at[around(4), core, pl.ds(32 * side, 32)]
        return send(place, place, z_sem, (7 + side,), plane_device(around(2 * side - 1)))

    def core_copy(plane, side):
        place = planes.at[plane, side]
        return send(place, place, core_sem, (plane,), other_core)

    core_copy(z, core).start()
    for step in (1, 2):
        z_copy(step).start()
    for copy in weights[2:6]:
        copy.wait()

    left, right = pl.ds(0, X_FIRST), pl.ds(X_FIRST, Y_FIRST)

    def part_x_copy(plane):
        return send(
            part.at[plane, 1 - x_lo, :, :, left], part_x.at[plane], part_sem, (plane, 0), other_x_lo
        )

    def part_y_copy(plane, step):
        return send(
            part.at[plane, :, y_at(step), :, right],
            part_y.at[plane, step - 1],
            part_sem,
            (plane, step),
            y_device(y_at(step)),
        )

    def mid_x_copy(plane, step):
        return send(
            mid_x.at[plane, y_at(step)],
            fin_x.at[plane, step - 1],
            part_sem,
            (plane, 3 + step),
            y_device(y_at(step)),
        )

    def mid_y_copy(plane):
        return send(mid_y.at[plane], fin_y.at[plane], part_sem, (plane, 7), other_x_lo)

    def straight_copy(step, ahead):
        image = image_at(ahead)
        return send(
            part.at[around(-offset_of(step)), image // STACK, image % STACK],
            straight_in.at[step - STAGED, dp],
            straight_sem,
            (step - STAGED, ahead),
            (image, mp),
        )

    def straight_landed(step, ahead):
        image = image_before(ahead)
        place = straight_in.at[step - STAGED, image]
        return send(place, place, straight_sem, (step - STAGED, ahead), (image, mp))

    def project(step):
        plane = around(-offset_of(step))
        core_copy(plane, 1 - core).wait_recv()
        rows = jnp.dot(
            to_strips(), planes[plane].reshape(BLOCK, WIDTH), preferred_element_type=F32
        ).astype(BF16)

        def block(columns, width):
            total = jnp.dot(rows, first[:, columns], preferred_element_type=F32)
            part[plane, :, :, :, columns] = total.astype(BF16).reshape(2, STACK, STRIP, width)

        block(left, X_FIRST)

        @pl.when(step < STAGED)
        def _():
            part_x_copy(plane).start()

        block(right, Y_FIRST)

        @pl.when(step < STAGED)
        def _():
            for ahead in FAR_FIRST:
                part_y_copy(plane, ahead).start()

        @pl.when(step >= STAGED)
        def _():
            for ahead in range(1, IMAGES):
                straight_copy(step, ahead).start()

        @pl.when(step + 1 < PLANES)
        def _():
            arrival = step + 1

            @pl.when(arrival < 7)
            def _():
                z_landed(arrival).wait_recv()

            @pl.when(arrival == 7)
            def _():
                for side in range(2):
                    z_half_landed(side).wait_recv()

            @pl.when(arrival < 5)
            def _():
                z_copy(arrival + 2).start()

            for side in range(2):

                @pl.when(arrival == 5 + side)
                def _():
                    z_half_copy(side).start()

            core_copy(around(-offset_of(arrival)), core).start()

    def halfway(step):
        plane = around(-offset_of(step))
        part_x_copy(plane).wait_recv()
        mid_x[plane] = (
            part[plane, x_lo, :, :, left].astype(F32) + part_x[plane].astype(F32)
        ).astype(BF16)
        for ahead in FAR_FIRST:
            mid_x_copy(plane, ahead).start()
        for ahead in range(1, STACK):
            part_y_copy(plane, ahead).wait_recv()

        def total(side):
            parts = [part_y[plane, slot, side].astype(F32) for slot in range(STACK - 1)]
            return part[plane, side, y, :, right].astype(F32) + parts[0] + parts[1] + parts[2]

        mid_y[plane] = total(1 - x_lo).astype(BF16)
        mid_y_copy(plane).start()
        keep_y[plane] = total(x_lo)

    def gelu(inner):
        return (0.5 * inner * (1.0 + lax.erf(inner * math.sqrt(0.5)))).astype(BF16)

    def collect(step):
        plane = around(-offset_of(step))
        for ahead in range(1, STACK):
            mid_x_copy(plane, ahead).wait_recv()
        total = mid_x[plane, y].astype(F32)
        for slot in range(STACK - 1):
            total += fin_x[plane, slot].astype(F32)
        strips[plane] = total[:, : 3 * HEAD].astype(BF16).astype(F32)
        cut = X_FIRST - 3 * HEAD
        acts[plane, x_lo, y, :, HEAD : HEAD + cut] = gelu(total[:, 3 * HEAD :] + bias[:cut])
        mid_y_copy(plane).wait_recv()
        total = keep_y[plane] + fin_y[plane].astype(F32)
        acts[plane, x_lo, y, :, HEAD + cut :] = gelu(total + bias[cut:])

    def collect_straight(step):
        plane = around(-offset_of(step))
        total = part[plane, x_lo, y].astype(F32)
        for ahead in range(1, IMAGES):
            straight_landed(step, ahead).wait_recv()
            total += straight_in[step - STAGED, image_before(ahead)].astype(F32)
        strips[plane] = total[:, : 3 * HEAD].astype(BF16).astype(F32)
        acts[plane, x_lo, y, :, HEAD:] = gelu(total[:, 3 * HEAD :] + bias[...])

    for copy in weights[6:8]:
        copy.wait()

    late = pl.ds(HEAD + X_ACTS, HIDDEN - X_ACTS)

    def mixed_copy(plane, step):
        place = acts.at[plane, x_lo, y, :, pl.ds(0, HEAD)]
        return send(place, place, mixed_sem, (plane, step), (image_at(step), mp))

    def mixed_landed(plane, step):
        image = image_before(step)
        place = acts.at[plane, image // STACK, image % STACK, :, pl.ds(0, HEAD)]
        return send(place, place, mixed_sem, (plane, step), (image, mp))

    def acts_x_copy(plane, side, low):
        place = acts.at[plane, side, y, :, pl.ds(low, HEAD + X_ACTS - low)]
        return send(place, place, acts_sem, (plane, 0), other_x_lo)

    def acts_y_copy(plane, step, low):
        place = acts.at[plane, x_lo, y, :, pl.ds(low, SECOND - low)]
        return send(place, place, acts_sem, (plane, step), y_device(y_at(step)))

    def acts_y_landed(plane, step, low):
        place = acts.at[plane, x_lo, y_before(step), :, pl.ds(low, SECOND - low)]
        return send(place, place, acts_sem, (plane, step), y_device(y_before(step)))

    def pass_y_copy(plane, step, low):
        place = acts.at[plane, 1 - x_lo, y, :, pl.ds(low, HEAD + X_ACTS - low)]
        return send(place, place, acts_sem, (plane, 3 + step), y_device(y_at(step)))

    def pass_y_landed(plane, step, low):
        place = acts.at[plane, 1 - x_lo, y_before(step), :, pl.ds(low, HEAD + X_ACTS - low)]
        return send(place, place, acts_sem, (plane, 3 + step), y_device(y_before(step)))

    def pass_x_copy(plane, side):
        place = acts.at[plane, side, :, :, late]
        return send(place, place, acts_sem, (plane, 7), other_x_lo)

    def far_first(step):
        return around(offset_of(PLANES - 1 - step))

    def spread(step, low):
        plane = far_first(step)
        acts_x_copy(plane, x_lo, low).start()
        for ahead in FAR_FIRST:
            acts_y_copy(plane, ahead, low).start()

    def spread_mixed(step):
        for ahead in range(1, IMAGES):
            mixed_copy(far_first(step), ahead).start()

    def pass_on(step, low):
        plane = far_first(step)
        acts_x_copy(plane, 1 - x_lo, low).wait_recv()
        for ahead in FAR_FIRST:
            pass_y_copy(plane, ahead, low).start()
        for ahead in range(1, STACK):
            acts_y_landed(plane, ahead, low).wait_recv()
        pass_x_copy(plane, x_lo).start()

    def landed(step, low):
        plane = far_first(step)
        for ahead in range(1, STACK):
            pass_y_landed(plane, ahead, low).wait_recv()
        pass_x_copy(plane, 1 - x_lo).wait_recv()

    def first_half(step, carry):
        @pl.when(step < PLANES)
        def _():
            project(step)

        @pl.when((step >= LAG) & (step < STAGED + LAG))
        def _():
            halfway(step - LAG)

        @pl.when(step == STAGED + LAG - 1)
        def _():
            for behind in range(AHEAD):
                spread(PLANES - 1 - behind, HEAD)

        @pl.when(step >= 2 * LAG)
        def _():
            collect(step - 2 * LAG)

        return carry

    lax.fori_loop(0, STAGED + 2 * LAG, first_half, 0)
    for step in range(STAGED, PLANES):
        collect_straight(step)

    for step in range(SOON):
        spread(step, HEAD)

    whole = strips[...].reshape(BLOCK, 3 * HEAD)
    query_norm = normalize(whole[:, :HEAD]).astype(BF16)
    key_norm = normalize(whole[:, HEAD : 2 * HEAD]).astype(BF16)
    scores = lax.dot_general(
        query_norm, key_norm, (((1,), (1,)), ((), ())), preferred_element_type=F32
    ) * (temper[...].reshape(1, 1) / math.sqrt(HEAD))
    weight = jnp.exp(scores - jnp.max(scores, axis=-1, keepdims=True))
    probs = (weight / jnp.sum(weight, axis=-1, keepdims=True)).astype(BF16)
    mixed = jnp.dot(probs, whole[:, 2 * HEAD :].astype(BF16), preferred_element_type=F32)
    mixed = mixed.astype(BF16).reshape(PLANES, STRIP, HEAD)
    for plane in range(PLANES):
        acts[plane, x_lo, y, :, :HEAD] = mixed[plane]
    for step in range(SOON):
        spread_mixed(step)

    def pair_copy(plane):
        return send(pair_out.at[plane], pair_in.at[plane], pair_sem, (plane,), other_core)

    def ring_way(step, side):
        return jnp.where(step == 0, 1 - 2 * side, -z_way(step))

    def ring_copy(step, side):
        return send(
            ring_out.at[step, side],
            ring_in.at[step, side],
            ring_sem,
            (step, side),
            plane_device(around(ring_way(step, side))),
        )

    def ring_landed(step, side):
        place = ring_in.at[step, side]
        return send(place, place, ring_sem, (step, side), plane_device(around(-ring_way(step, side))))

    def output(step):
        plane = far_first(step)

        @pl.when((step < SOON) | (step >= PLANES - AHEAD))
        def _():
            landed(step, HEAD)
            for ahead in range(1, IMAGES):
                mixed_landed(plane, ahead).wait_recv()

        @pl.when((step >= SOON) & (step < PLANES - AHEAD))
        def _():
            landed(step, 0)

        rows = jnp.dot(
            from_strips(), acts[plane].reshape(BLOCK, SECOND), preferred_element_type=F32
        ).astype(BF16)
        block = jnp.dot(rows, second[...], preferred_element_type=F32).reshape(2, 2, 32, WIDTH)
        pair_out[plane] = jnp.where(core == 0, block[1], block[0]).astype(BF16)
        pair_copy(plane).start()
        pair_own[plane] = jnp.where(core == 0, block[0], block[1])

    def merge(step):
        plane = around(offset_of(PLANES - 1 - step))
        pair_copy(plane).wait_recv()
        for side in range(2):
            pair_own[plane, side] = pair_own[plane, side] + pair_in[plane, side].astype(F32)

            @pl.when((step >= 3) | (step == 2 - side))
            def _():
                before = jnp.maximum(step - 2, 0)
                ring_landed(before, side).wait_recv()
                pair_own[plane, side] = pair_own[plane, side] + ring_in[before, side].astype(F32)

            @pl.when(step < PLANES - 1)
            def _():
                ring_out[step, side] = pair_own[plane, side].astype(BF16)
                ring_copy(step, side).start()

    for copy in weights[8:]:
        copy.wait()

    def second_half(step, carry):
        @pl.when(step < PLANES - AHEAD - SOON)
        def _():
            spread(step + SOON, 0)

        @pl.when((step >= PLANES - AHEAD - SOON) & (step < PLANES - SOON))
        def _():
            spread_mixed(step + SOON)

        @pl.when((step < SOON) | ((step >= PLANES - AHEAD) & (step < PLANES)))
        def _():
            pass_on(step, HEAD)

        @pl.when((step >= SOON) & (step < PLANES - AHEAD))
        def _():
            pass_on(step, 0)

        @pl.when((step >= SOON) & (step < PLANES + SOON))
        def _():
            output(step - SOON)

        @pl.when(step >= SOON + 1)
        def _():
            merge(step - SOON - 1)

        return carry

    lax.fori_loop(0, PLANES + SOON + 1, second_half, 0)
    for side in range(2):
        ring_landed(6, side).wait_recv()
        lines[pl.ds(32 * side, 32), :] = pair_own[z, side] + ring_in[6, side].astype(F32)
    for side in range(2):
        for image in range(IMAGES):
            final_out[side, image] = lines[pl.ds(side * 32 + image * ROWS, ROWS), :].astype(BF16)

    def final_copy(step, flip):
        return send(
            final_out.at[half(flip), image_at(step)],
            final_in.at[dp, x_hi],
            final_sem,
            (step, flip),
            (image_at(step), half_mp(flip)),
        )

    def final_landed(step, flip):
        place = final_in.at[image_before(step), half(flip)]
        return send(place, place, final_sem, (step, flip), (image_before(step), half_mp(flip)))

    for piece in pieces:
        final_copy(*piece).start()
    final_in[dp, x_hi] = final_out[x_hi, dp]
    for piece in pieces:
        final_landed(*piece).wait_recv()
    for block in range(IMAGES):
        columns = pl.ds(block * WIDTH, WIDTH)
        total = final_in[block, 0].astype(F32) + final_in[block, 1].astype(F32)
        out[:, columns] = (tokens[:, columns].astype(F32) + total).astype(BF16)

    for step in range(PLANES):
        plane = far_first(step)
        low = 0 if SOON <= step < PLANES - AHEAD else HEAD
        acts_x_copy(plane, x_lo, low).wait_send()
        for ahead in range(1, STACK):
            acts_y_copy(plane, ahead, low).wait_send()
            pass_y_copy(plane, ahead, low).wait_send()
        if low:
            for ahead in range(1, IMAGES):
                mixed_copy(plane, ahead).wait_send()
    for piece in pieces:
        norm_copy(*piece).wait_send()
        final_copy(*piece).wait_send()
    for step in range(1, 7):
        z_copy(step).wait_send()
    for side in range(2):
        z_half_copy(side).wait_send()
        for step in range(PLANES - 1):
            ring_copy(step, side).wait_send()

    def sent(step, carry):
        plane = around(-offset_of(step))
        core_copy(plane, core).wait_send()
        pair_copy(plane).wait_send()
        pass_x_copy(plane, x_lo).wait_send()

        @pl.when(step < STAGED)
        def _():
            part_x_copy(plane).wait_send()
            mid_y_copy(plane).wait_send()
            for ahead in range(1, STACK):
                part_y_copy(plane, ahead).wait_send()
                mid_x_copy(plane, ahead).wait_send()

        @pl.when(step >= STAGED)
        def _():
            for ahead in range(1, IMAGES):
                straight_copy(step, ahead).wait_send()

        return carry

    lax.fori_loop(0, PLANES, sent, 0)


def per_device(
    tokens, norm_gain, w_query, w_key, w_value, w_inner, bias_inner, w_attn_out, w_outer, temper
):
    vmem = pl.BlockSpec(memory_space=pltpu.VMEM)
    hbm = pl.BlockSpec(memory_space=pltpu.HBM)
    dma = pltpu.SemaphoreType.DMA
    return pl.pallas_call(
        kernel,
        out_shape=jax.ShapeDtypeStruct(tokens.shape, BF16),
        in_specs=[hbm] * 10,
        out_specs=vmem,
        scratch_shapes=[
            pltpu.VMEM((ROWS, IMAGES * WIDTH), BF16),
            pltpu.VMEM((1, IMAGES * WIDTH), F32),
            pltpu.VMEM((HIDDEN,), F32),
            pltpu.VMEM((1,), F32),
            pltpu.VMEM((WIDTH, FIRST), BF16),
            pltpu.VMEM((SECOND, WIDTH), BF16),
            pltpu.VMEM((IMAGES, ROWS, WIDTH), BF16),
            pltpu.VMEM((IMAGES, 2, ROWS, WIDTH), BF16),
            pltpu.VMEM((64, WIDTH), F32),
            pltpu.VMEM((PLANES, 2, 64, WIDTH), BF16),
            pltpu.VMEM((PLANES, 2, STACK, STRIP, FIRST), BF16),
            pltpu.VMEM((PLANES, STACK, STRIP, X_FIRST), BF16),
            pltpu.VMEM((PLANES, STACK, STRIP, X_FIRST), BF16),
            pltpu.VMEM((PLANES, STACK - 1, STRIP, X_FIRST), BF16),
            pltpu.VMEM((PLANES, STACK - 1, 2, STRIP, Y_FIRST), BF16),
            pltpu.VMEM((PLANES, STRIP, Y_FIRST), BF16),
            pltpu.VMEM((PLANES, STRIP, Y_FIRST), F32),
            pltpu.VMEM((PLANES, STRIP, Y_FIRST), BF16),
            pltpu.VMEM((STRAIGHT, IMAGES, STRIP, FIRST), BF16),
            pltpu.VMEM((PLANES, STRIP, 3 * HEAD), F32),
            pltpu.VMEM((PLANES, 2, STACK, STRIP, SECOND), BF16),
            pltpu.VMEM((PLANES, 2, 32, WIDTH), F32),
            pltpu.VMEM((PLANES, 2, 32, WIDTH), BF16),
            pltpu.VMEM((PLANES, 2, 32, WIDTH), BF16),
            pltpu.VMEM((PLANES - 1, 2, 32, WIDTH), BF16),
            pltpu.VMEM((PLANES - 1, 2, 32, WIDTH), BF16),
            pltpu.VMEM((2, IMAGES, ROWS, WIDTH), BF16),
            pltpu.VMEM((IMAGES, 2, ROWS, WIDTH), BF16),
            dma((10,)),
            dma((2, IMAGES, 2)),
            dma((2, 9)),
            dma((2, PLANES)),
            dma((2, PLANES, 8)),
            dma((2, STRAIGHT, IMAGES)),
            dma((2, PLANES, 8)),
            dma((2, PLANES, IMAGES)),
            dma((2, PLANES)),
            dma((2, PLANES - 1, 2)),
            dma((2, IMAGES, 2)),
        ],
        compiler_params=pltpu.CompilerParams(
            collective_id=0, has_side_effects=True, vmem_limit_bytes=67043328
        ),
    )(
        tokens,
        norm_gain.reshape(1, -1),
        w_query,
        w_key,
        w_value,
        w_inner,
        bias_inner,
        w_attn_out,
        w_outer,
        temper,
    )


def solution(mesh):
    return jax.shard_map(
        per_device,
        mesh=mesh,
        in_specs=(
            P(("dp", "mp"), None),
            P(),
            P("dp", "mp"),
            P("dp", "mp"),
            P("dp", "mp"),
            P("dp", "mp"),
            P("mp"),
            P("mp", "dp"),
            P("mp", "dp"),
            P("mp"),
        ),
        out_specs=P(("dp", "mp"), None),
        check_vma=False,
    )
```
